32 devices in a mesh: ctx: 8 (over z, core), tp: 4 (over y, x).
Axes of the slice: x: 2, y: 2, z: 4, core: 2. Of those that a mesh axis runs over, the one named last changes fastest.
Arguments:
- act_codes: bfloat16 [2048, 4096], P(('ctx', 'tp')), may hold values from -6 to 6
- scale_exps: int32 [2048, 32], P(('ctx', 'tp')), may hold values from -2 to 2
- weight: bfloat16 [4096, 6144], P(None, 'tp'), may hold values from -0.09375 to 0.09375
- grad_out: bfloat16 [2048, 6144], P('ctx', 'tp'), may hold values from -6 to 6
Outputs:
- grad_input: bfloat16 [2048, 4096], P(('ctx', 'tp'))
- grad_weight: float32 [4096, 6144], P('ctx', 'tp')
The draws below stay inside these ranges and needn't reach their ends.
All inputs are finite; a program needn't handle non-finite values.
Results may differ from the reference program's by a relative error of at most 0.023.
Values may be sent and summed in bfloat16 or wider, within the bound.
A program may use at most 64 MiB of HBM per device.

```python
import jax
import jax.numpy as jnp
from jax import lax

D = 4096
BLOCK = 128
QKVW = 6144
TOKENS = 2048
N_TP = 4


def plant(array, own_key, least, high):
    place = [jax.random.randint(jax.random.fold_in(own_key, axis), (), 0, length) for axis, length in enumerate(array.shape)]
    longest = array.shape.index(max(array.shape))
    neighbour = place[:longest] + [(place[longest] + 1) % array.shape[longest]] + place[longest + 1:]
    return array.at[tuple(place)].set(least).at[tuple(neighbour)].set(high)


def strengthened(array, own_key, source, target, parts, factor):
    owner, partner = [(jnp.arange(array.shape[axis_at]) // (array.shape[axis_at] // parts)).reshape([-1 if axis == axis_at else 1 for axis in range(array.ndim)]) for axis_at in (source, target)]
    chosen = jax.random.permutation(own_key, parts)[partner]
    strong = (owner == chosen) | (owner == (partner + parts // 2) % parts)
    return jnp.where(strong, factor * array, array)


def levels(stream_key, shape, shards, low, top_value):
    loudness, own = 1.0, jax.random.fold_in(stream_key, 6)
    for position, parts in shards:
        steps = jnp.exp(jax.random.uniform(jax.random.fold_in(own, position), (parts,), jnp.float32, low / len(shards), top_value / len(shards)))
        loudness = loudness * jnp.repeat(steps, shape[position] // parts).reshape([-1 if axis == position else 1 for axis in range(len(shape))])
    return loudness


def gaussian(own_key, dims, deviation, reach, cuts=(), kind=jnp.bfloat16):
    values = jax.random.normal(own_key, dims, jnp.float32) * deviation
    if len(cuts) > 0:
        values = levels(own_key, dims, cuts, -0.22, 0.18) * values
    return jnp.clip(values, min=-reach, max=reach).astype(kind)


def noise_with(stream_key, extent, scale, reach, pieces, heavy, held_as=jnp.bfloat16):
    drawn = scale * jax.random.normal(stream_key, extent, jnp.float32)
    if pieces:
        drawn = drawn * levels(stream_key, extent, pieces, -0.22, 0.18)
    return jnp.clip(strengthened(drawn, jax.random.fold_in(stream_key, 3), *heavy), -reach, reach).astype(held_as)


def setup_inputs(seed: int = 0) -> dict:
    key_list = jax.random.split(jax.random.key(seed), 5)
    act_codes = noise_with(key_list[0], (TOKENS, D), 1.0, 6.0, ((0, 32),), (0, 1, 32, 2.75))
    scale_exps = plant(jax.random.randint(key_list[1], (TOKENS, D // BLOCK), -2, 3), jax.random.fold_in(key_list[1], 1), -2, 2).astype(jnp.int32)
    weight = gaussian(key_list[2], (D, QKVW), D ** -0.5, 0.09375, ((1, 4),))
    grad_out = noise_with(key_list[3], (TOKENS, QKVW), 1.0, 6.0, ((0, 8), (1, 4)), (1, 0, 8, 2.0))
    return {"act_codes": act_codes, "scale_exps": scale_exps, "weight": weight, "grad_out": grad_out}


def dequantize(act_codes, scale_exps):
    tok_rows = act_codes.shape[0]
    scales = jnp.exp2(scale_exps.astype(jnp.float32))
    blocked = act_codes.astype(jnp.float32).reshape(tok_rows, D // BLOCK, BLOCK) * scales[:, :, None]
    return blocked.reshape(tok_rows, D).astype(jnp.bfloat16)

def reference(act_codes, scale_exps, weight, grad_out):
    acts = dequantize(act_codes, scale_exps)
    grad_weight = jnp.dot(acts.T, grad_out, preferred_element_type=jnp.float32)
    grad_weight = grad_weight * lax.rsqrt(jnp.float32(TOKENS))
    width = QKVW // N_TP

    def add_block(total, index):
        offset = (index * width).astype(jnp.int32)
        grads = lax.dynamic_slice_in_dim(grad_out, offset, width, 1)
        weights = lax.dynamic_slice_in_dim(weight, offset, width, 1)
        part = lax.dot_general(grads, weights, (((1,), (1,)), ((), ())), preferred_element_type=jnp.float32)
        part = lax.optimization_barrier(part.astype(jnp.bfloat16))
        return (total + part.astype(jnp.float32), None)
    total, unused = lax.scan(add_block, jnp.zeros((TOKENS, D), jnp.float32), jnp.arange(N_TP, dtype=jnp.int32))
    return (total.astype(jnp.bfloat16), grad_weight)
```

```python
import functools

import jax
import jax.numpy as jnp
from jax import lax
from jax.experimental import pallas as pl
from jax.experimental.pallas import tpu as pltpu
from jax.sharding import PartitionSpec as P

MESH = pl.DeviceIdType.MESH
CHUNKS = 4


def line_kernel(
    n_ctx, n_tp, tokens,
    codes_hbm, exps_hbm, weight_ref, grads_ref,
    gin_ref, gw_ref,
    codes_ref, exps_ref, w_buf, g_buf, a_send, a_buf, part, landed,
    in_sem, w_sem, g_sem,
    a_ssem, a_rsem, b_ssem, b_rsem, up_ssem, down_ssem, mate_ssem, g_rsem, p_ssem, p_rsem,
):
    n_line = n_ctx // 2
    me = lax.axis_index("ctx")
    tp = lax.axis_index("tp")
    core = lax.rem(me, 2)
    z = lax.div(me, 2)
    mate = me + 1 - 2 * core
    rows, width = codes_ref.shape
    block = width // exps_ref.shape[0]
    feats = width // n_ctx
    d_tile = w_buf.shape[1]
    n_d = w_buf.shape[0]
    scale = lax.rsqrt(jnp.float32(tokens))
    split = n_ctx * n_tp <= 64

    def load_w(i):
        return pltpu.make_async_copy(
            weight_ref.at[pl.ds(i * d_tile, d_tile)], w_buf.at[i], w_sem.at[i]
        )

    def load_g(k):
        size = g_buf.shape[2]
        return pltpu.make_async_copy(
            grads_ref.at[pl.ds(k * size, size)], g_buf.at[me, k], g_sem.at[k]
        )

    load_codes = pltpu.make_async_copy(codes_hbm, codes_ref, in_sem.at[0])
    load_exps = pltpu.make_async_copy(exps_hbm, exps_ref, in_sem.at[1])
    load_g(0).start()
    load_codes.start()
    load_exps.start()
    for k in range(1, CHUNKS):
        load_g(k).start()
    for i in range(n_d):
        load_w(i).start()

    barrier = pltpu.get_barrier_semaphore()
    for r in range(1, n_ctx):
        pl.semaphore_signal(
            barrier, inc=1, device_id=(lax.rem(me + r, n_ctx), tp), device_id_type=MESH
        )
    for r in range(1, n_tp):
        pl.semaphore_signal(
            barrier, inc=1, device_id=(me, lax.rem(tp + r, n_tp)), device_id_type=MESH
        )

    pl.semaphore_wait(barrier, n_ctx + n_tp - 2)

    def remote(src, dst, ssem, rsem, to):
        return pltpu.make_async_remote_copy(
            src_ref=src, dst_ref=dst, send_sem=ssem, recv_sem=rsem,
            device_id=to, device_id_type=MESH,
        )

    def act_copy(to):
        return remote(
            a_send.at[to], a_buf.at[me, tp], a_ssem.at[to], a_rsem.at[me], (to, tp)
        )

    def act_landing(source):
        return remote(
            a_send.at[source], a_buf.at[source, tp], a_ssem.at[source], a_rsem.at[source],
            (source, tp),
        )

    def spread_copy(s, q, src=None):
        return remote(
            a_buf.at[s, tp] if src is None else src,
            a_buf.at[s, tp], b_ssem.at[s, q], b_rsem.at[s, tp], (me, q),
        )

    def spread_landing(s, q):
        return remote(
            a_buf.at[s, q], a_buf.at[s, q], b_ssem.at[s, q], b_rsem.at[s, q], (me, q)
        )

    def spread_all(q):
        return remote(
            a_buf.at[:, tp], a_buf.at[:, tp], b_ssem.at[0, q], b_rsem.at[0, tp], (me, q)
        )

    def spread_all_landing(q):
        return remote(
            a_buf.at[:, q], a_buf.at[:, q], b_ssem.at[0, q], b_rsem.at[0, q], (me, q)
        )

    def pass_on(s, k, ssem, to):
        return remote(
            g_buf.at[s, k], g_buf.at[s, k], ssem.at[lax.div(s, 2), k], g_rsem.at[s, k], (to, tp)
        )

    def up(s, k):
        return pass_on(s, k, up_ssem, me + 2)

    def down(s, k):
        return pass_on(s, k, down_ssem, me - 2)

    def across(s, k):
        return pass_on(s, k, mate_ssem, mate)

    has_up = z < n_line - 1
    has_down = z > 0

    def send_own(k):
        load_g(k).wait()

        @pl.when(has_up)
        def _():
            up(me, k).start()

        @pl.when(has_down)
        def _():
            down(me, k).start()

        across(me, k).start()

    send_own(0)
    load_codes.wait()
    load_exps.wait()
    powers = jnp.exp2(exps_ref[...].astype(jnp.float32)).T
    for b in range(width // block):
        owner, place = divmod(b * block, feats)
        value = codes_ref[:, b * block : (b + 1) * block].astype(jnp.float32)
        value = value * powers[:, b : b + 1]
        a_send[owner, :, place : place + block] = value.astype(jnp.bfloat16)
    a_buf[me, tp] = a_send[me]
    for r in range(1, n_ctx):
        act_copy(lax.rem(me + r, n_ctx)).start()
    for k in range(1, CHUNKS):
        send_own(k)

    peers = [lax.rem(tp + r, n_tp) for r in range(1, n_tp)]
    if split:
        for q in peers:
            spread_copy(me, q, a_send.at[me]).start()

    grads = g_buf.at[me]

    def part_piece(i):
        load_w(i).wait()
        rows_all = grads[...].reshape(-1, g_buf.shape[3])
        piece = lax.dot_general(
            rows_all, w_buf[i], (((1,), (1,)), ((), ())), preferred_element_type=jnp.float32
        ).astype(jnp.bfloat16)
        part[:, :, i * d_tile : (i + 1) * d_tile] = piece.reshape(n_tp, rows, d_tile)

    per = -(-n_d // n_ctx)
    done = 0
    for r in range(1, n_ctx):
        for i in range(done, min(done + per, n_d)):
            part_piece(i)
        done = min(done + per, n_d)
        s = lax.rem(me - r + n_ctx, n_ctx)
        act_landing(s).wait_recv()
        if split:
            for q in peers:
                spread_copy(s, q).start()
    for i in range(done, n_d):
        part_piece(i)
    if not split:
        for q in peers:
            spread_all(q).start()

    def part_copy(q):
        return remote(part.at[q], landed.at[tp], p_ssem.at[q], p_rsem.at[tp], (me, q))

    def part_landing(q):
        return remote(part.at[q], landed.at[q], p_ssem.at[q], p_rsem.at[q], (me, q))

    for q in peers:
        part_copy(q).start()

    n_cols = g_buf.shape[3]
    n_tile = 512 if n_cols % 512 == 0 else n_cols

    def accumulate(zz, first, k=None):
        if k is None:
            lhs = a_buf[pl.ds(2 * zz, 2)].reshape(-1, feats).T
        else:
            size = n_tp // CHUNKS
            lhs = a_buf[pl.ds(2 * zz, 2), k * size : (k + 1) * size].reshape(-1, feats).T

        for j in range(n_cols // n_tile):
            cols = slice(j * n_tile, (j + 1) * n_tile)
            if k is None:
                rhs = g_buf[pl.ds(2 * zz, 2), :, :, cols].reshape(-1, n_tile)
            else:
                rhs = g_buf[pl.ds(2 * zz, 2), k, :, cols].reshape(-1, n_tile)
            term = jnp.dot(lhs, rhs, preferred_element_type=jnp.float32) * scale
            if first:
                gw_ref[:, cols] = term
            else:
                gw_ref[:, cols] += term

    def await_acts(zz, first):
        if split:
            for c in range(2):
                for q in peers:
                    spread_landing(2 * zz + c, q).wait_recv()
        elif first:
            for q in peers:
                spread_all_landing(q).wait_recv()

    def chip_terms(zz, first=False):
        other = 2 * zz + 1 - core
        for k in range(CHUNKS):
            across(other, k).wait_recv()
        await_acts(zz, first)
        accumulate(zz, first)

    def terms_at(d):
        if d == 0:
            chip_terms(z, True)
            return

        @pl.when(z >= d)
        def _():
            chip_terms(z - d)

        @pl.when(z + d < n_line)
        def _():
            chip_terms(z + d)

    def sum_parts():
        for q in peers:
            part_landing(q).wait_recv()
        total = part[tp].astype(jnp.float32)
        for q in peers:
            total = total + landed[q].astype(jnp.float32)
        gin_ref[...] = total.astype(jnp.bfloat16)

    def from_below(d, k):
        s = me - 2 * d
        up(s, k).wait_recv()

        @pl.when(has_up)
        def _():
            up(s, k).start()

        across(s, k).start()

    def from_above(d, k):
        s = me + 2 * d
        down(s, k).wait_recv()

        @pl.when(has_down)
        def _():
            down(s, k).start()

        across(s, k).start()

    for d in range(1, n_line - 1):
        for k in range(CHUNKS):

            @pl.when(z >= d)
            def _():
                from_below(d, k)

            @pl.when(z + d < n_line)
            def _():
                from_above(d, k)

        terms_at(d - 1)

    d = n_line - 1
    terms_at(d - 1)

    def last_terms(zz, arrive):
        other = 2 * zz + 1 - core
        await_acts(zz, False)
        for k in range(CHUNKS):
            arrive(d, k)
            if k == CHUNKS - 1:
                sum_parts()
            if k > 0:
                across(other, k - 1).wait_recv()
                accumulate(zz, False, k - 1)
        across(other, CHUNKS - 1).wait_recv()
        accumulate(zz, False, CHUNKS - 1)

    @pl.when(z == d)
    def _():
        last_terms(0, from_below)

    @pl.when(z == 0)
    def _():
        last_terms(d, from_above)

    @pl.when((z > 0) & (z < d))
    def _():
        sum_parts()

    for r in range(1, n_ctx):
        act_copy(lax.rem(me + r, n_ctx)).wait_send()
    for q in peers:
        part_copy(q).wait_send()
        if split:
            for s in range(n_ctx):
                spread_copy(s, q).wait_send()
        else:
            spread_all(q).wait_send()
    for zz in range(n_line):
        for k in range(CHUNKS):
            s = 2 * zz + core
            across(s, k).wait_send()

            @pl.when(has_up & (zz <= z))
            def _():
                up(s, k).wait_send()

            @pl.when(has_down & (zz >= z))
            def _():
                down(s, k).wait_send()


def line_body(act_codes, scale_exps, weight, grad_out):
    n_ctx, n_tp = lax.axis_size("ctx"), lax.axis_size("tp")
    n_line = n_ctx // 2
    rows, width = act_codes.shape
    toks, cols = grad_out.shape
    feats = width // n_ctx
    d_tile = min(512, width)
    dma = pltpu.SemaphoreType.DMA
    lanes = -(-cols // 128) * 128
    outs = -(-rows // 16) * 16 * width * 2 + feats * lanes * 4
    vmem = pl.BlockSpec(memory_space=pltpu.VMEM)
    hbm = pl.BlockSpec(memory_space=pltpu.HBM)
    bf16 = jnp.bfloat16
    return pl.pallas_call(
        functools.partial(line_kernel, n_ctx, n_tp, toks * n_ctx),
        out_shape=(
            pltpu.VMEM((rows, width), bf16),
            pltpu.VMEM((feats, cols), jnp.float32),
        ),
        in_specs=[hbm, hbm, hbm, hbm],
        out_specs=(vmem, vmem),
        scratch_shapes=[
            pltpu.VMEM((rows, width), bf16),
            pltpu.VMEM(scale_exps.shape[::-1], scale_exps.dtype),
            pltpu.VMEM((width // d_tile, d_tile, cols), bf16),
            pltpu.VMEM((n_ctx, CHUNKS, toks // CHUNKS, cols), bf16),
            pltpu.VMEM((n_ctx, rows, feats), bf16),
            pltpu.VMEM((n_ctx, n_tp, rows, feats), bf16),
            pltpu.VMEM((n_tp, rows, width), bf16),
            pltpu.VMEM((n_tp, rows, width), bf16),
            dma((2,)),
            dma((width // d_tile,)),
            dma((CHUNKS,)),
            dma((n_ctx,)),
            dma((n_ctx,)),
            dma((n_ctx if n_ctx * n_tp <= 64 else 1, n_tp)),
            dma((n_ctx if n_ctx * n_tp <= 64 else 1, n_tp)),
            dma((n_line, CHUNKS)),
            dma((n_line, CHUNKS)),
            dma((n_line, CHUNKS)),
            dma((n_ctx, CHUNKS)),
            dma((n_tp,)),
            dma((n_tp,)),
        ],
        compiler_params=pltpu.CompilerParams(
            collective_id=0, has_side_effects=True, vmem_limit_bytes=67_043_328 - outs - 8192
        ),
    )(act_codes, scale_exps.T, weight, grad_out)


RAW = 1
WIDE = 256


def blocks_of(cols):
    full = cols // WIDE - 1
    return [(b * WIDE, WIDE) for b in range(full)] + [
        (full * WIDE + i * (WIDE // 2), WIDE // 2) for i in range(2)
    ]


def square_kernel(
    n_ctx, n_tp, tokens,
    codes_hbm, exps_hbm, weight_ref, grads_ref,
    gin_ref, gw_ref,
    codes_ref, exps_ref, w_buf, g_own, g_wide, g_slim, a_send, a_buf, p_buf, a_t, p_t,
    part, recv1, total1, recv2, sums_out, sums_in, slim_out, slim_in,
    in_sem, w_sem, g_sem,
    a_ssem, a_rsem, p_rsem, fwd_ssem, spread_ssem, g_ssem, g_rsem,
    one_ssem, one_rsem, two_ssem, two_rsem, s_ssem, s_rsem,
):
    me = lax.axis_index("ctx")
    tp = lax.axis_index("tp")
    core = lax.rem(me, 2)
    z = lax.div(me, 2)
    mate = me + 1 - 2 * core
    n_line = n_ctx // 2
    side = lax.div(z, 2)
    z_end, z_mid = (n_line - 1) * side, 1 + side
    z_far_mid, z_far_end = 2 - side, (n_line - 1) * (1 - side)
    y, x = lax.div(tp, 2), lax.rem(tp, 2)
    by_x, by_y = 2 * y + 1 - x, 2 * (1 - y) + x
    near = by_x + core * (by_y - by_x)
    next_ = by_y + core * (by_x - by_y)
    diag = n_tp - 1 - tp
    rows, width = codes_ref.shape
    toks = g_own.shape[0]
    block = width // exps_ref.shape[0]
    feats = width // n_ctx
    d_tile = w_buf.shape[1]
    n_d = w_buf.shape[0]
    chip = 2 * toks
    scale = lax.rsqrt(jnp.float32(tokens))
    blocks = blocks_of(g_own.shape[1])
    n_b = len(blocks)
    full = n_b - 2

    def g_at(b):
        return g_wide.at[b] if b < full else g_slim.at[b - full]

    def g_piece(s, b):
        return g_at(b).at[pl.ds(s * toks, toks)]

    def load_w(i):
        return pltpu.make_async_copy(
            weight_ref.at[pl.ds(i * d_tile, d_tile)], w_buf.at[i], w_sem.at[i]
        )

    def load_g(b):
        start, size = blocks[b]
        return pltpu.make_async_copy(
            grads_ref.at[:, pl.ds(start, size)], g_piece(me, b), g_sem.at[b]
        )

    load_codes = pltpu.make_async_copy(codes_hbm, codes_ref, in_sem.at[0])
    load_exps = pltpu.make_async_copy(exps_hbm, exps_ref, in_sem.at[1])
    load_own = pltpu.make_async_copy(grads_ref, g_own, in_sem.at[2])
    load_g(0).start()
    load_codes.start()
    load_exps.start()
    load_g(1).start()
    load_own.start()
    load_w(0).start()
    for b in range(2, n_b):
        load_g(b).start()
    for i in range(1, n_d):
        load_w(i).start()

    barrier = pltpu.get_barrier_semaphore()
    for r in range(1, n_ctx):
        pl.semaphore_signal(
            barrier, inc=1, device_id=(lax.rem(me + r, n_ctx), tp), device_id_type=MESH
        )
    for r in range(1, n_tp):
        pl.semaphore_signal(
            barrier, inc=1, device_id=(me, lax.rem(tp + r, n_tp)), device_id_type=MESH
        )
    pl.semaphore_wait(barrier, n_ctx + n_tp - 2)

    def dequantize():
        load_codes.wait()
        load_exps.wait()
        powers = jnp.exp2(exps_ref[...].astype(jnp.float32)).T
        for b in range(width // block):
            owner, place = divmod(b * block, feats)
            value = codes_ref[:, b * block : (b + 1) * block].astype(jnp.float32)
            value = value * powers[:, b : b + 1]
            a_send[owner, :, place : place + block] = value.astype(jnp.bfloat16)
        a_buf[me, tp] = a_send[me]

    def program(is_mid):
        pending = []

        def send(src, dst, ssem, rsem, to):
            copy = pltpu.make_async_remote_copy(
                src_ref=src, dst_ref=dst, send_sem=ssem, recv_sem=rsem,
                device_id=to, device_id_type=MESH,
            )
            copy.start()
            pending.append(copy)

        def landed(dst, ssem, rsem):
            pltpu.make_async_remote_copy(
                src_ref=dst, dst_ref=dst, send_sem=ssem, recv_sem=rsem,
                device_id=(me, tp), device_id_type=MESH,
            ).wait_recv()

        def both(zz):
            return (2 * zz, 2 * zz + 1)

        acts, ends = (a_buf, a_rsem, 0), (p_buf, p_rsem, 1)

        def act_send(d, to, kind):
            buf, rsem, _ = kind
            send(a_send.at[d], buf.at[me, tp], a_ssem.at[d], rsem.at[me, tp], (to, tp))

        def spread(kind, s):
            buf, rsem, k = kind
            for n, q in enumerate((near, next_)):
                send(buf.at[s, tp], buf.at[s, tp], spread_ssem.at[k, s, n], rsem.at[s, tp], (me, q))

        def pass_end(s):
            send(
                p_buf.at[s, tp], a_buf.at[s, tp], fwd_ssem.at[s], a_rsem.at[s, tp],
                (2 * z_end + core, tp),
            )

        def arrive(kind, s):
            buf, rsem, k = kind
            landed(buf.at[s, tp], spread_ssem.at[k, s, 0], rsem.at[s, tp])
            spread(kind, s)
            if k == 1:
                pass_end(s)

        def relay(kind, s):
            buf, rsem, k = kind
            landed(buf.at[s, near], spread_ssem.at[k, s, 2], rsem.at[s, near])
            send(
                buf.at[s, near], buf.at[s, near], spread_ssem.at[k, s, 2], rsem.at[s, near],
                (me, next_),
            )

        def gathered(kind, s):
            buf, rsem, k = kind
            for q in (next_, diag):
                landed(buf.at[s, q], spread_ssem.at[k, s, 2], rsem.at[s, q])

        def turn(kind, zz):
            buf, _, k = kind
            for s in both(zz):
                gathered(kind, s)
            value = buf[pl.ds(2 * zz, 2)].reshape(chip, feats).T
            if k == 0:
                a_t[:, pl.ds(pl.multiple_of(zz * chip, chip), chip)] = value
            else:
                p_t[:, pl.ds(pl.multiple_of((zz - 1 + side) * chip, chip), chip)] = value

        def g_send(s, b, way, to):
            send(
                g_piece(s, b), g_piece(s, b), g_ssem.at[way, lax.div(s, 2), b], g_rsem.at[s, b],
                (to, tp),
            )

        inward = 2 * (z_far_mid if is_mid else z_mid) + core
        outward = 2 * z_end + core

        def g_await(s, b):
            landed(g_piece(s, b), g_ssem.at[0, 0, b], g_rsem.at[s, b])

        def g_mine(b):
            load_g(b).wait()
            g_send(me, b, 0, inward)
            if is_mid and b < RAW:
                g_send(me, b, 1, outward)
            g_send(me, b, 2, mate)

        def g_take(zz, b, on):
            s = 2 * zz + core
            g_await(s, b)
            if on is not None:
                g_send(s, b, on, inward if on == 0 else outward)
            g_send(s, b, 2, mate)

        def g_mates(zs, b):
            for zz in zs:
                g_await(2 * zz + 1 - core, b)

        def piece(i):
            if i == 0:
                load_own.wait()
            load_w(i).wait()
            value = lax.dot_general(
                g_own[...], w_buf[i], (((1,), (1,)), ((), ())), preferred_element_type=jnp.float32
            ).astype(jnp.bfloat16)
            value = value.reshape(n_tp, rows, d_tile)
            for q in range(n_tp):
                dy, dx = lax.rem(y + q // 2, 2), lax.rem(x + q % 2, 2)
                slot = 2 * dx + dy + core * (dy - dx)
                part[i, slot] = value[q]

        def part_one(i):
            send(part.at[i, pl.ds(2, 2)], recv1.at[i], one_ssem.at[i], one_rsem.at[i], (me, near))

        def part_two(i):
            landed(recv1.at[i], one_ssem.at[i], one_rsem.at[i])
            total = part[i, 1].astype(jnp.float32) + recv1[i, 1].astype(jnp.float32)
            total1[i] = total.astype(jnp.bfloat16)
            send(total1.at[i], recv2.at[i], two_ssem.at[i], two_rsem.at[i], (me, next_))

        def part_sum(i):
            landed(recv2.at[i], two_ssem.at[i], two_rsem.at[i])
            total = part[i, 0].astype(jnp.float32) + recv1[i, 0].astype(jnp.float32)
            total = total + recv2[i].astype(jnp.float32)
            gin_ref[:, i * d_tile : (i + 1) * d_tile] = total.astype(jnp.bfloat16)

        def dot(lhs, rhs):
            return jnp.dot(lhs, rhs, preferred_element_type=jnp.float32)

        def cols(b):
            start, size = blocks[b]
            return slice(start, start + size)

        def whole_block(b):
            gw_ref[:, cols(b)] = dot(a_t[...], g_at(b)[...]) * scale

        def out_at(b):
            return sums_out.at[b - RAW] if b < full else slim_out.at[b - full]

        def in_at(b):
            return sums_in.at[b - RAW] if b < full else slim_in.at[b - full]

        def sum_block(b):
            first = pl.multiple_of((1 - side) * chip, chip)
            rhs = g_at(b)[pl.ds(first, (n_line - 1) * chip)]
            out_at(b)[...] = dot(p_t[...], rhs).astype(jnp.bfloat16)
            send(out_at(b), in_at(b), s_ssem.at[b], s_rsem.at[b], (outward, tp))

        def own_block(b):
            here = pl.ds(pl.multiple_of(z_end * chip, chip), chip)
            gw_ref[:, cols(b)] = dot(a_t[:, here], g_at(b)[here])

        def add_block(b):
            landed(in_at(b), s_ssem.at[b], s_rsem.at[b])
            gw_ref[:, cols(b)] = (gw_ref[:, cols(b)] + in_at(b)[...].astype(jnp.float32)) * scale

        others = (z_mid, z_far_mid, z_far_end)
        g_mine(0)
        dequantize()
        if is_mid:
            p_buf[me, tp] = a_send[2 * z_end + core]
            for c in range(2):
                act_send(2 * z_far_end + c, 2 * z_far_mid + c, ends)
            pass_end(me)
            act_send(2 * z_end + 1 - core, mate, ends)
            spread(ends, me)
            g_mine(1)
            for c in range(2):
                act_send(2 * z_far_mid + c, 2 * z_far_mid + c, acts)
            act_send(mate, mate, acts)
            spread(acts, me)
            piece(0)
            arrive(ends, mate)
            arrive(acts, mate)
            piece(1)
            relay(ends, me)
            relay(ends, mate)
            piece(2)
            relay(acts, me)
            relay(acts, mate)
            piece(3)
            for s in both(z_far_mid):
                arrive(ends, s)
            piece(4)
            g_take(z_end, 0, 0)
            for s in both(z_far_end):
                arrive(ends, s)
            piece(5)
            for s in both(z_far_mid):
                relay(ends, s)
            piece(6)
            piece(7)
            for s in both(z_far_end):
                relay(ends, s)
            g_take(z_far_mid, 0, 1)
            g_take(z_end, 1, 0)
            g_mine(2)
            for i in range(4):
                part_one(i)
            for zz in (z_end, z_far_mid, z_far_end):
                for s in both(zz):
                    arrive(acts, s)
            for i in range(4, n_d):
                part_one(i)
            for zz in (z_end, z_far_mid, z_far_end):
                for s in both(zz):
                    relay(acts, s)
            for zz in others:
                turn(ends, zz)
            g_take(z_far_end, 0, 1)
            for zz in (z_mid, z_end, z_far_mid, z_far_end):
                turn(acts, zz)
            for b in range(n_b):
                if b > 0:
                    if b + 1 < n_b:
                        g_take(z_end, b + 1, 0)
                    if b + 2 < n_b:
                        g_mine(b + 2)
                    g_take(z_far_mid, b, 1 if b < RAW else None)
                    g_take(z_far_end, b, 1 if b < RAW else None)
                g_mates((z_mid, z_end, z_far_mid, z_far_end), b)
                if b >= RAW:
                    sum_block(b)
                whole_block(b)
                if 0 < b < 5:
                    part_two(2 * b - 2)
                    part_two(2 * b - 1)
                if b == 5:
                    for i in range(n_d):
                        part_sum(i)
        else:
            for c in range(2):
                act_send(2 * z_far_end + c, 2 * z_far_mid + c, ends)
            g_mine(1)
            spread(acts, me)
            act_send(mate, mate, acts)
            for c in range(2):
                act_send(2 * z_far_mid + c, 2 * z_far_mid + c, acts)
            for c in range(2):
                act_send(2 * z_mid + c, 2 * z_mid + c, acts)
            for b in range(2, n_b):
                g_mine(b)
            piece(0)
            arrive(acts, mate)
            piece(1)
            relay(acts, me)
            relay(acts, mate)
            piece(2)
            for s in both(z_mid):
                arrive(acts, s)
            piece(3)
            piece(4)
            for s in both(z_mid):
                relay(acts, s)
            g_take(z_mid, 0, None)
            piece(5)
            for s in both(z_far_mid):
                arrive(acts, s)
            piece(6)
            piece(7)
            for i in range(4):
                part_one(i)
            for s in both(z_far_end):
                arrive(acts, s)
            for i in range(4, n_d):
                part_one(i)
            for zz in (z_far_mid, z_far_end):
                for s in both(zz):
                    relay(acts, s)
            turn(acts, z_end)
            for b in range(RAW, n_b):
                g_mates((z_end,), b)
                own_block(b)
            g_take(z_far_mid, 0, None)
            for i in range(n_d // 2):
                part_two(i)
            for zz in others:
                turn(acts, zz)
            g_take(z_far_end, 0, None)
            g_mates((z_end,) + others, 0)
            whole_block(0)
            for i in range(n_d // 2, n_d):
                part_two(i)
            for b in range(RAW, n_b):
                add_block(b)
                if b == n_b - 3:
                    for i in range(n_d):
                        part_sum(i)
        for copy in pending:
            copy.wait_send()

    is_mid = (z == z_mid)

    @pl.when(is_mid)
    def _():
        program(True)

    @pl.when(jnp.logical_not(is_mid))
    def _():
        program(False)


def square_body(act_codes, scale_exps, weight, grad_out):
    n_ctx, n_tp = lax.axis_size("ctx"), lax.axis_size("tp")
    rows, width = act_codes.shape
    toks, cols = grad_out.shape
    feats = width // n_ctx
    d_tile = width // 8
    n_d = width // d_tile
    all_toks = toks * n_ctx
    n_b = len(blocks_of(cols))
    full = n_b - 2
    dma = pltpu.SemaphoreType.DMA
    vmem = pl.BlockSpec(memory_space=pltpu.VMEM)
    hbm = pl.BlockSpec(memory_space=pltpu.HBM)
    bf16 = jnp.bfloat16
    outs = rows * width * 2 + feats * cols * 4
    return pl.pallas_call(
        functools.partial(square_kernel, n_ctx, n_tp, all_toks),
        out_shape=(
            pltpu.VMEM((rows, width), bf16),
            pltpu.VMEM((feats, cols), jnp.float32),
        ),
        in_specs=[hbm, hbm, hbm, hbm],
        out_specs=(vmem, vmem),
        scratch_shapes=[
            pltpu.VMEM((rows, width), bf16),
            pltpu.VMEM(scale_exps.shape[::-1], scale_exps.dtype),
            pltpu.VMEM((n_d, d_tile, cols), bf16),
            pltpu.VMEM((toks, cols), bf16),
            pltpu.VMEM((full, all_toks, WIDE), bf16),
            pltpu.VMEM((2, all_toks, WIDE // 2), bf16),
            pltpu.VMEM((n_ctx, rows, feats), bf16),
            pltpu.VMEM((n_ctx, n_tp, rows, feats), bf16),
            pltpu.VMEM((n_ctx, n_tp, rows, feats), bf16),
            pltpu.VMEM((feats, all_toks), bf16),
            pltpu.VMEM((feats, all_toks - 2 * toks), bf16),
            pltpu.VMEM((n_d, n_tp, rows, d_tile), bf16),
            pltpu.VMEM((n_d, 2, rows, d_tile), bf16),
            pltpu.VMEM((n_d, rows, d_tile), bf16),
            pltpu.VMEM((n_d, rows, d_tile), bf16),
            pltpu.VMEM((full - RAW, feats, WIDE), bf16),
            pltpu.VMEM((full - RAW, feats, WIDE), bf16),
            pltpu.VMEM((2, feats, WIDE // 2), bf16),
            pltpu.VMEM((2, feats, WIDE // 2), bf16),
            dma((3,)),
            dma((n_d,)),
            dma((n_b,)),
            dma((n_ctx,)),
            dma((n_ctx, n_tp)),
            dma((n_ctx, n_tp)),
            dma((n_ctx,)),
            dma((2, n_ctx, 3)),
            dma((3, n_ctx // 2, n_b)),
            dma((n_ctx, n_b)),
            dma((n_d,)),
            dma((n_d,)),
            dma((n_d,)),
            dma((n_d,)),
            dma((n_b,)),
            dma((n_b,)),
        ],
        compiler_params=pltpu.CompilerParams(
            collective_id=0, has_side_effects=True, vmem_limit_bytes=67_043_328 - outs - 8192
        ),
    )(act_codes, scale_exps.T, weight, grad_out)


def body(act_codes, scale_exps, weight, grad_out):
    line, square = lax.axis_size("ctx") // 2, lax.axis_size("tp")
    if line == 4 and square == 4 and grad_out.shape[1] % WIDE == 0:
        return square_body(act_codes, scale_exps, weight, grad_out)
    return line_body(act_codes, scale_exps, weight, grad_out)


def solution(mesh):
    placed = (P(("ctx", "tp"), None), P(("ctx", "tp"), None), P(None, "tp"), P("ctx", "tp"))
    return jax.shard_map(
        body,
        mesh=mesh,
        in_specs=placed,
        out_specs=(P(("ctx", "tp"), None), P("ctx", "tp")),
        check_vma=False,
    )
```

```python
import functools
import math

import jax
import jax.numpy as jnp
from jax import lax
from jax.experimental import pallas as pl
from jax.experimental.pallas import tpu as pltpu
from jax.sharding import PartitionSpec as P

MESH = pl.DeviceIdType.MESH
CHUNKS = 4


def line_kernel(
    n_ctx, n_tp, tokens,
    codes_hbm, exps_hbm, weight_ref, grads_ref,
    gin_ref, gw_ref,
    codes_ref, exps_ref, w_buf, g_buf, a_send, a_buf, part, landed,
    in_sem, w_sem, g_sem,
    a_ssem, a_rsem, b_ssem, b_rsem, up_ssem, down_ssem, mate_ssem, g_rsem, p_ssem, p_rsem,
):
    n_line = n_ctx // 2
    me = lax.axis_index("ctx")
    tp = lax.axis_index("tp")
    core = lax.rem(me, 2)
    z = lax.div(me, 2)
    mate = me + 1 - 2 * core
    rows, width = codes_ref.shape
    block = width // exps_ref.shape[0]
    feats = width // n_ctx
    d_tile = w_buf.shape[1]
    n_d = w_buf.shape[0]
    scale = lax.rsqrt(jnp.float32(tokens))
    split = n_ctx * n_tp <= 64

    def load_w(i):
        return pltpu.make_async_copy(
            weight_ref.at[pl.ds(i * d_tile, d_tile)], w_buf.at[i], w_sem.at[i]
        )

    def load_g(k):
        size = g_buf.shape[2]
        return pltpu.make_async_copy(
            grads_ref.at[pl.ds(k * size, size)], g_buf.at[me, k], g_sem.at[k]
        )

    load_codes = pltpu.make_async_copy(codes_hbm, codes_ref, in_sem.at[0])
    load_exps = pltpu.make_async_copy(exps_hbm, exps_ref, in_sem.at[1])
    load_g(0).start()
    load_codes.start()
    load_exps.start()
    for k in range(1, CHUNKS):
        load_g(k).start()
    for i in range(n_d):
        load_w(i).start()

    barrier = pltpu.get_barrier_semaphore()
    for r in range(1, n_ctx):
        pl.semaphore_signal(
            barrier, inc=1, device_id=(lax.rem(me + r, n_ctx), tp), device_id_type=MESH
        )
    for r in range(1, n_tp):
        pl.semaphore_signal(
            barrier, inc=1, device_id=(me, lax.rem(tp + r, n_tp)), device_id_type=MESH
        )

    pl.semaphore_wait(barrier, n_ctx + n_tp - 2)

    def remote(src, dst, ssem, rsem, to):
        return pltpu.make_async_remote_copy(
            src_ref=src, dst_ref=dst, send_sem=ssem, recv_sem=rsem,
            device_id=to, device_id_type=MESH,
        )

    def act_copy(to):
        return remote(
            a_send.at[to], a_buf.at[me, tp], a_ssem.at[to], a_rsem.at[me], (to, tp)
        )

    def act_landing(source):
        return remote(
            a_send.at[source], a_buf.at[source, tp], a_ssem.at[source], a_rsem.at[source],
            (source, tp),
        )

    def spread_copy(s, q, src=None):
        return remote(
            a_buf.at[s, tp] if src is None else src,
            a_buf.at[s, tp], b_ssem.at[s, q], b_rsem.at[s, tp], (me, q),
        )

    def spread_landing(s, q):
        return remote(
            a_buf.at[s, q], a_buf.at[s, q], b_ssem.at[s, q], b_rsem.at[s, q], (me, q)
        )

    def spread_all(q):
        return remote(
            a_buf.at[:, tp], a_buf.at[:, tp], b_ssem.at[0, q], b_rsem.at[0, tp], (me, q)
        )

    def spread_all_landing(q):
        return remote(
            a_buf.at[:, q], a_buf.at[:, q], b_ssem.at[0, q], b_rsem.at[0, q], (me, q)
        )

    def pass_on(s, k, ssem, to):
        return remote(
            g_buf.at[s, k], g_buf.at[s, k], ssem.at[lax.div(s, 2), k], g_rsem.at[s, k], (to, tp)
        )

    def up(s, k):
        return pass_on(s, k, up_ssem, me + 2)

    def down(s, k):
        return pass_on(s, k, down_ssem, me - 2)

    def across(s, k):
        return pass_on(s, k, mate_ssem, mate)

    has_up = z < n_line - 1
    has_down = z > 0

    def send_own(k):
        load_g(k).wait()

        @pl.when(has_up)
        def _():
            up(me, k).start()

        @pl.when(has_down)
        def _():
            down(me, k).start()

        across(me, k).start()

    send_own(0)
    load_codes.wait()
    load_exps.wait()
    powers = jnp.exp2(exps_ref[...].astype(jnp.float32)).T
    for b in range(width // block):
        owner, place = divmod(b * block, feats)
        value = codes_ref[:, b * block : (b + 1) * block].astype(jnp.float32)
        value = value * powers[:, b : b + 1]
        a_send[owner, :, place : place + block] = value.astype(jnp.bfloat16)
    a_buf[me, tp] = a_send[me]
    for r in range(1, n_ctx):
        act_copy(lax.rem(me + r, n_ctx)).start()
    for k in range(1, CHUNKS):
        send_own(k)

    peers = [lax.rem(tp + r, n_tp) for r in range(1, n_tp)]
    if split:
        for q in peers:
            spread_copy(me, q, a_send.at[me]).start()

    grads = g_buf.at[me]

    def part_piece(i):
        load_w(i).wait()
        rows_all = grads[...].reshape(-1, g_buf.shape[3])
        piece = lax.dot_general(
            rows_all, w_buf[i], (((1,), (1,)), ((), ())), preferred_element_type=jnp.float32
        ).astype(jnp.bfloat16)
        part[:, :, i * d_tile : (i + 1) * d_tile] = piece.reshape(n_tp, rows, d_tile)

    per = -(-n_d // n_ctx)
    done = 0
    for r in range(1, n_ctx):
        for i in range(done, min(done + per, n_d)):
            part_piece(i)
        done = min(done + per, n_d)
        s = lax.rem(me - r + n_ctx, n_ctx)
        act_landing(s).wait_recv()
        if split:
            for q in peers:
                spread_copy(s, q).start()
    for i in range(done, n_d):
        part_piece(i)
    if not split:
        for q in peers:
            spread_all(q).start()

    def part_copy(q):
        return remote(part.at[q], landed.at[tp], p_ssem.at[q], p_rsem.at[tp], (me, q))

    def part_landing(q):
        return remote(part.at[q], landed.at[q], p_ssem.at[q], p_rsem.at[q], (me, q))

    for q in peers:
        part_copy(q).start()

    n_cols = g_buf.shape[3]
    n_tile = 512 if n_cols % 512 == 0 else n_cols

    def accumulate(zz, first, k=None):
        if k is None:
            lhs = a_buf[pl.ds(2 * zz, 2)].reshape(-1, feats).T
        else:
            size = n_tp // CHUNKS
            lhs = a_buf[pl.ds(2 * zz, 2), k * size : (k + 1) * size].reshape(-1, feats).T

        for j in range(n_cols // n_tile):
            cols = slice(j * n_tile, (j + 1) * n_tile)
            if k is None:
                rhs = g_buf[pl.ds(2 * zz, 2), :, :, cols].reshape(-1, n_tile)
            else:
                rhs = g_buf[pl.ds(2 * zz, 2), k, :, cols].reshape(-1, n_tile)
            term = jnp.dot(lhs, rhs, preferred_element_type=jnp.float32) * scale
            if first:
                gw_ref[:, cols] = term
            else:
                gw_ref[:, cols] += term

    def await_acts(zz, first):
        if split:
            for c in range(2):
                for q in peers:
                    spread_landing(2 * zz + c, q).wait_recv()
        elif first:
            for q in peers:
                spread_all_landing(q).wait_recv()

    def chip_terms(zz, first=False):
        other = 2 * zz + 1 - core
        for k in range(CHUNKS):
            across(other, k).wait_recv()
        await_acts(zz, first)
        accumulate(zz, first)

    def terms_at(d):
        if d == 0:
            chip_terms(z, True)
            return

        @pl.when(z >= d)
        def _():
            chip_terms(z - d)

        @pl.when(z + d < n_line)
        def _():
            chip_terms(z + d)

    def sum_parts():
        for q in peers:
            part_landing(q).wait_recv()
        total = part[tp].astype(jnp.float32)
        for q in peers:
            total = total + landed[q].astype(jnp.float32)
        gin_ref[...] = total.astype(jnp.bfloat16)

    def from_below(d, k):
        s = me - 2 * d
        up(s, k).wait_recv()

        @pl.when(has_up)
        def _():
            up(s, k).start()

        across(s, k).start()

    def from_above(d, k):
        s = me + 2 * d
        down(s, k).wait_recv()

        @pl.when(has_down)
        def _():
            down(s, k).start()

        across(s, k).start()

    for d in range(1, n_line - 1):
        for k in range(CHUNKS):

            @pl.when(z >= d)
            def _():
                from_below(d, k)

            @pl.when(z + d < n_line)
            def _():
                from_above(d, k)

        terms_at(d - 1)

    d = n_line - 1
    terms_at(d - 1)

    def last_terms(zz, arrive):
        other = 2 * zz + 1 - core
        await_acts(zz, False)
        for k in range(CHUNKS):
            arrive(d, k)
            if k == CHUNKS - 1:
                sum_parts()
            if k > 0:
                across(other, k - 1).wait_recv()
                accumulate(zz, False, k - 1)
        across(other, CHUNKS - 1).wait_recv()
        accumulate(zz, False, CHUNKS - 1)

    @pl.when(z == d)
    def _():
        last_terms(0, from_below)

    @pl.when(z == 0)
    def _():
        last_terms(d, from_above)

    @pl.when((z > 0) & (z < d))
    def _():
        sum_parts()

    for r in range(1, n_ctx):
        act_copy(lax.rem(me + r, n_ctx)).wait_send()
    for q in peers:
        part_copy(q).wait_send()
        if split:
            for s in range(n_ctx):
                spread_copy(s, q).wait_send()
        else:
            spread_all(q).wait_send()
    for zz in range(n_line):
        for k in range(CHUNKS):
            s = 2 * zz + core
            across(s, k).wait_send()

            @pl.when(has_up & (zz <= z))
            def _():
                up(s, k).wait_send()

            @pl.when(has_down & (zz >= z))
            def _():
                down(s, k).wait_send()


def line_body(act_codes, scale_exps, weight, grad_out):
    n_ctx, n_tp = lax.axis_size("ctx"), lax.axis_size("tp")
    n_line = n_ctx // 2
    rows, width = act_codes.shape
    toks, cols = grad_out.shape
    feats = width // n_ctx
    d_tile = min(512, width)
    dma = pltpu.SemaphoreType.DMA
    lanes = -(-cols // 128) * 128
    outs = -(-rows // 16) * 16 * width * 2 + feats * lanes * 4
    vmem = pl.BlockSpec(memory_space=pltpu.VMEM)
    hbm = pl.BlockSpec(memory_space=pltpu.HBM)
    bf16 = jnp.bfloat16
    return pl.pallas_call(
        functools.partial(line_kernel, n_ctx, n_tp, toks * n_ctx),
        out_shape=(
            pltpu.VMEM((rows, width), bf16),
            pltpu.VMEM((feats, cols), jnp.float32),
        ),
        in_specs=[hbm, hbm, hbm, hbm],
        out_specs=(vmem, vmem),
        scratch_shapes=[
            pltpu.VMEM((rows, width), bf16),
            pltpu.VMEM(scale_exps.shape[::-1], scale_exps.dtype),
            pltpu.VMEM((width // d_tile, d_tile, cols), bf16),
            pltpu.VMEM((n_ctx, CHUNKS, toks // CHUNKS, cols), bf16),
            pltpu.VMEM((n_ctx, rows, feats), bf16),
            pltpu.VMEM((n_ctx, n_tp, rows, feats), bf16),
            pltpu.VMEM((n_tp, rows, width), bf16),
            pltpu.VMEM((n_tp, rows, width), bf16),
            dma((2,)),
            dma((width // d_tile,)),
            dma((CHUNKS,)),
            dma((n_ctx,)),
            dma((n_ctx,)),
            dma((n_ctx if n_ctx * n_tp <= 64 else 1, n_tp)),
            dma((n_ctx if n_ctx * n_tp <= 64 else 1, n_tp)),
            dma((n_line, CHUNKS)),
            dma((n_line, CHUNKS)),
            dma((n_line, CHUNKS)),
            dma((n_ctx, CHUNKS)),
            dma((n_tp,)),
            dma((n_tp,)),
        ],
        compiler_params=pltpu.CompilerParams(
            collective_id=0, has_side_effects=True, vmem_limit_bytes=67_043_328 - outs - 8192
        ),
    )(act_codes, scale_exps.T, weight, grad_out)


RAW = 2
WIDE = 256


def wide_blocks(cols):
    return cols // WIDE * 3 // 6


def blocks_of(cols):
    full = wide_blocks(cols)
    slim = WIDE // 2
    return [(b * WIDE, WIDE) for b in range(full)] + [
        (start, slim) for start in range(full * WIDE, cols, slim)
    ]


def square_kernel(
    n_ctx, n_tp, tokens,
    codes_hbm, exps_hbm, weight_ref, grads_ref,
    gin_ref, gw_ref,
    codes_ref, exps_ref, w_buf, g_own, g_wide, g_slim, a_send, a_buf, p_buf, a_t, p_t,
    part, recv1, total1, recv2, sums_out, sums_in, slim_out, slim_in,
    in_sem, w_sem, g_sem, s_sem, line_sem, near_sem, rest_sem, g_rsem, mate_sem,
    one_sem, two_sem, sum_sem,
):
    me = lax.axis_index("ctx")
    tp = lax.axis_index("tp")
    core = lax.rem(me, 2)
    z = lax.div(me, 2)
    mate = me + 1 - 2 * core
    n_line = n_ctx // 2
    side = lax.div(z, 2)
    z_end, z_mid = (n_line - 1) * side, 1 + side
    z_far_mid, z_far_end = 2 - side, (n_line - 1) * (1 - side)
    y, x = lax.div(tp, 2), lax.rem(tp, 2)
    by_x, by_y = 2 * y + 1 - x, 2 * (1 - y) + x
    near = by_x + core * (by_y - by_x)
    next_ = by_y + core * (by_x - by_y)
    diag = n_tp - 1 - tp
    rows, width = codes_ref.shape
    toks = g_own.shape[0]
    block = width // exps_ref.shape[0]
    feats = width // n_ctx
    d_tile = w_buf.shape[1]
    n_d = w_buf.shape[0]
    chip = 2 * toks
    unit = rows * feats
    scale = lax.rsqrt(jnp.float32(tokens))
    blocks = blocks_of(g_own.shape[1])
    n_b = len(blocks)
    full = g_wide.shape[0]

    def g_at(b):
        return g_wide.at[b] if b < full else g_slim.at[b - full]

    def g_piece(s, b):
        return g_at(b).at[pl.ds(s * toks, toks)]

    def load_w(i):
        return pltpu.make_async_copy(
            weight_ref.at[pl.ds(i * d_tile, d_tile)], w_buf.at[i], w_sem.at[i % 2]
        )

    def load_g(b):
        start, size = blocks[b]
        return pltpu.make_async_copy(
            grads_ref.at[:, pl.ds(start, size)], g_piece(me, b), g_sem.at[b]
        )

    load_codes = pltpu.make_async_copy(codes_hbm, codes_ref, in_sem.at[0])
    load_exps = pltpu.make_async_copy(exps_hbm, exps_ref, in_sem.at[1])
    load_own = pltpu.make_async_copy(grads_ref, g_own, in_sem.at[2])
    load_codes.start()
    load_exps.start()
    load_g(0).start()
    load_g(1).start()

    barrier = pltpu.get_barrier_semaphore()
    for r in range(1, n_ctx):
        pl.semaphore_signal(
            barrier, inc=1, device_id=(lax.rem(me + r, n_ctx), tp), device_id_type=MESH
        )
    for r in range(1, n_tp):
        pl.semaphore_signal(
            barrier, inc=1, device_id=(me, lax.rem(tp + r, n_tp)), device_id_type=MESH
        )
    load_exps.wait()
    load_codes.wait()
    load_own.start()
    load_w(0).start()
    for b in range(2, n_b):
        load_g(b).start()
    load_w(1).start()
    powers = jnp.exp2(exps_ref[...].astype(jnp.float32)).T
    for b in range(width // block):
        owner, place = divmod(b * block, feats)
        value = codes_ref[:, b * block : (b + 1) * block].astype(jnp.float32)
        value = value * powers[:, b : b + 1]
        a_send[owner, :, place : place + block] = value.astype(jnp.bfloat16)
    a_buf[me, tp] = a_send[me]
    p_buf[me, tp] = a_send[2 * (z_mid + z_end - z) + core]
    pl.semaphore_wait(barrier, n_ctx + n_tp - 2)

    def program(is_mid):
        sent = {}

        def remote(src, dst, ssem, rsem, to):
            return pltpu.make_async_remote_copy(
                src_ref=src, dst_ref=dst, send_sem=ssem, recv_sem=rsem,
                device_id=to, device_id_type=MESH,
            )

        def send(kind, src, dst, rsem, to):
            remote(src, dst, s_sem.at[kind], rsem, to).start()
            sent[kind] = sent.get(kind, 0) + math.prod(src.shape) // unit

        def landed(dst, rsem):
            remote(dst, dst, s_sem.at[0], rsem, (me, tp)).wait_recv()

        def all_sent():
            for kind, n in sent.items():
                if n % 24 == 0:
                    ref = w_buf.at[pl.ds(0, n // 24)]
                elif n % 2 == 0 and n // 2 <= n_d:
                    ref = recv1.at[pl.ds(0, n // 2)]
                elif n <= n_d:
                    ref = recv2.at[pl.ds(0, n)]
                else:
                    ref = a_buf.at[pl.ds(0, n // n_tp)]
                assert math.prod(ref.shape) == n * unit
                remote(ref, ref, s_sem.at[kind], near_sem.at[0, 0], (me, tp)).wait_send()

        def both(zz):
            return (2 * zz, 2 * zz + 1)

        acts, ends = (a_buf, 0), (p_buf, 1)

        def act_send(d, to, kind):
            buf, k = kind
            send(0, a_send.at[d], buf.at[me, tp], line_sem.at[k, me], (to, tp))

        def spread(kind, s):
            buf, k = kind
            send(1, buf.at[s, tp], buf.at[s, tp], near_sem.at[k, s], (me, near))
            send(2, buf.at[s, tp], buf.at[s, tp], rest_sem.at[k, lax.div(s, 2)], (me, next_))

        def pass_end(s):
            send(3, p_buf.at[s, tp], a_buf.at[s, tp], line_sem.at[0, s], (2 * z_end + core, tp))

        def arrive(kind, s):
            buf, k = kind
            landed(buf.at[s, tp], line_sem.at[k, s])
            spread(kind, s)
            if k == 1 and is_mid:
                pass_end(s)

        def relay(kind, s):
            buf, k = kind
            landed(buf.at[s, near], near_sem.at[k, s])
            send(4, buf.at[s, near], buf.at[s, near], rest_sem.at[k, lax.div(s, 2)], (me, next_))

        def gathered(kind, zz):
            buf, k = kind
            landed(buf.at[2 * zz], rest_sem.at[k, zz])

        def pass_back(s, q):
            send(
                3, p_buf.at[s, q], a_buf.at[s, q], rest_sem.at[0, lax.div(s, 2)],
                (2 * z_mid + core, tp),
            )

        def turned(kind, zz):
            buf, k = kind
            value = buf[pl.ds(2 * zz, 2)].reshape(chip, feats).T
            if k == 0:
                a_t[:, pl.ds(pl.multiple_of(zz * chip, chip), chip)] = value
            else:
                p_t[:, pl.ds(pl.multiple_of((zz - 1 + side) * chip, chip), chip)] = value

        def turn(kind, zz):
            gathered(kind, zz)
            turned(kind, zz)

        def turn_whole(zz):
            landed(a_buf.at[pl.ds(2 * zz, 2)], rest_sem.at[0, zz])
            turned(acts, zz)

        def g_send(kind, s, b, rsem, to):
            send(kind, g_piece(s, b), g_piece(s, b), rsem, (to, tp))

        inward = 2 * (z_far_mid if is_mid else z_mid) + core
        outward = 2 * z_end + core
        FROM_SIDE, FROM_MID, FROM_END = 0, 1, 2

        def g_mine(b):
            load_g(b).wait()
            g_send(5, me, b, g_rsem.at[FROM_MID if is_mid else FROM_SIDE, b], inward)
            if is_mid and b < RAW:
                g_send(6, me, b, g_rsem.at[FROM_SIDE, b], outward)
            g_send(7, me, b, mate_sem.at[b], mate)

        def g_take(zz, way, b):
            s = 2 * zz + core
            landed(g_piece(s, b), g_rsem.at[way, b])
            if is_mid and way == FROM_SIDE:
                g_send(5, s, b, g_rsem.at[FROM_END, b], inward)
            elif is_mid and b < RAW:
                g_send(6, s, b, g_rsem.at[way, b], outward)
            g_send(7, s, b, mate_sem.at[b], mate)

        def g_mates(n, b):
            landed(g_at(b).at[pl.ds(0, n * toks)], mate_sem.at[b])

        def piece(i):
            if i == 0:
                load_own.wait()
            load_w(i).wait()
            if i + 2 < n_d:
                load_w(i + 2).start()
            value = lax.dot_general(
                g_own[...], w_buf[i], (((1,), (1,)), ((), ())), preferred_element_type=jnp.float32
            ).astype(jnp.bfloat16)
            value = value.reshape(n_tp, rows, d_tile)
            for q in range(n_tp):
                dy, dx = lax.rem(y + q // 2, 2), lax.rem(x + q % 2, 2)
                slot = 2 * dx + dy + core * (dy - dx)
                part[i, slot] = value[q]

        def part_one(i):
            send(8, part.at[i, pl.ds(2, 2)], recv1.at[i], one_sem.at[i], (me, near))

        def part_two(i):
            landed(recv1.at[i], one_sem.at[i])
            total = part[i, 1].astype(jnp.float32) + recv1[i, 1].astype(jnp.float32)
            total1[i] = total.astype(jnp.bfloat16)
            send(9, total1.at[i], recv2.at[i], two_sem.at[i], (me, next_))

        def part_sum(i):
            landed(recv2.at[i], two_sem.at[i])
            total = part[i, 0].astype(jnp.float32) + recv1[i, 0].astype(jnp.float32)
            total = total + recv2[i].astype(jnp.float32)
            gin_ref[:, i * d_tile : (i + 1) * d_tile] = total.astype(jnp.bfloat16)

        def dot(lhs, rhs):
            return jnp.dot(lhs, rhs, preferred_element_type=jnp.float32)

        halves = [slice(h * (feats // 2), (h + 1) * (feats // 2)) for h in range(2)]

        def cols(b):
            start, size = blocks[b]
            return slice(start, start + size)

        def whole_block(b):
            for half in halves:
                gw_ref[half, cols(b)] = dot(a_t[half], g_at(b)[...]) * scale

        def whole_pair(b):
            start, size = blocks[b]
            for half in halves:
                rhs = jnp.concatenate([g_at(b)[...], g_at(b + 1)[...]], axis=1)
                gw_ref[half, start : start + 2 * size] = dot(a_t[half], rhs) * scale

        def out_at(b):
            return sums_out.at[b - RAW] if b < full else slim_out.at[b - full]

        def in_at(b):
            return sums_in.at[b - RAW] if b < full else slim_in.at[b - full]

        def sum_block(b):
            first = pl.multiple_of((1 - side) * chip, chip)
            for half in halves:
                rhs = g_at(b)[pl.ds(first, (n_line - 1) * chip)]
                out_at(b)[half] = dot(p_t[half], rhs).astype(jnp.bfloat16)
                send(10, out_at(b).at[half], in_at(b).at[half], sum_sem.at[b], (outward, tp))

        def own_block(b):
            here = pl.ds(pl.multiple_of(z_end * chip, chip), chip)
            for half in halves:
                gw_ref[half, cols(b)] = dot(a_t[half, here], g_at(b)[here])

        def add_block(b):
            landed(in_at(b), sum_sem.at[b])
            gw_ref[:, cols(b)] = (gw_ref[:, cols(b)] + in_at(b)[...].astype(jnp.float32)) * scale

        if is_mid:
            g_mine(7)
            g_mine(3)
            for c in range(2):
                act_send(2 * z_far_end + c, 2 * z_far_mid + c, ends)
            g_mine(1)
            pass_end(me)
            act_send(2 * z_end + 1 - core, mate, ends)
            spread(ends, me)
            act_send(mate, mate, acts)
            spread(acts, me)
            piece(0)
            piece(1)
            arrive(acts, mate)
            arrive(ends, mate)
            piece(2)
            piece(3)
            piece(4)
            piece(5)
            g_take(z_far_mid, FROM_MID, 7)
            relay(ends, me)
            piece(6)
            piece(7)
            g_take(z_far_mid, FROM_MID, 3)
            relay(acts, me)
            arrive(ends, 2 * z_far_mid + core)
            relay(acts, mate)
            arrive(ends, 2 * z_far_mid + 1 - core)
            relay(ends, mate)
            g_take(z_end, FROM_SIDE, 0)
            g_mine(0)
            g_take(z_end, FROM_SIDE, 2)
            g_mine(2)
            relay(ends, 2 * z_far_mid + core)
            g_take(z_far_mid, FROM_MID, 1)
            relay(ends, 2 * z_far_mid + 1 - core)
            turn(acts, z_mid)
            part_one(0)
            arrive(ends, 2 * z_far_end + core)
            turn(ends, z_mid)
            turn(ends, z_far_mid)
            arrive(ends, 2 * z_far_end + 1 - core)
            g_take(z_far_end, FROM_END, 0)
            part_two(0)
            relay(ends, 2 * z_far_end + core)
            part_one(1)
            part_one(2)
            g_take(z_far_mid, FROM_MID, 0)
            part_one(3)
            g_take(z_end, FROM_SIDE, 3)
            g_mine(4)
            g_mine(5)
            relay(ends, 2 * z_far_end + 1 - core)
            part_one(4)
            g_mates(n_line, 0)
            g_take(z_end, FROM_SIDE, 5)
            g_take(z_end, FROM_SIDE, 4)
            part_sum(0)
            part_one(5)
            g_take(z_far_end, FROM_END, 2)
            part_one(6)
            part_two(1)
            turn(ends, z_far_end)
            g_take(z_far_mid, FROM_MID, 2)
            g_take(z_end, FROM_SIDE, 6)
            g_mine(6)
            for c in range(2):
                act_send(2 * z_far_mid + c, 2 * z_far_mid + c, acts)
            part_two(2)
            g_mates(n_line, 2)
            sum_block(2)
            g_take(z_far_end, FROM_END, 3)
            part_two(3)
            part_sum(1)
            g_take(z_far_mid, FROM_MID, 4)
            g_mates(n_line, 3)
            sum_block(3)
            g_take(z_far_mid, FROM_MID, 5)
            part_sum(2)
            part_two(4)
            g_take(z_far_end, FROM_END, 5)
            g_take(z_end, FROM_SIDE, 7)
            g_take(z_end, FROM_SIDE, 1)
            g_take(z_end, FROM_SIDE, 8)
            g_mine(8)
            part_one(7)
            part_sum(3)
            part_two(5)
            g_mates(n_line, 5)
            g_take(z_far_end, FROM_END, 4)
            g_mates(n_line, 4)
            sum_block(4)
            part_two(6)
            part_sum(4)
            sum_block(5)
            g_take(z_far_end, FROM_END, 6)
            part_sum(5)
            part_two(7)
            g_take(z_far_mid, FROM_MID, 6)
            arrive(acts, 2 * z_far_end + core)
            part_sum(6)
            g_mates(n_line, 6)
            sum_block(6)
            arrive(acts, 2 * z_far_mid + core)
            part_sum(7)
            arrive(acts, 2 * z_far_end + 1 - core)
            arrive(acts, 2 * z_far_mid + 1 - core)
            turn_whole(z_end)
            relay(acts, 2 * z_far_end + core)
            g_take(z_far_end, FROM_END, 7)
            relay(acts, 2 * z_far_mid + core)
            g_mates(n_line, 7)
            sum_block(7)
            relay(acts, 2 * z_far_end + 1 - core)
            g_take(z_far_end, FROM_END, 1)
            relay(acts, 2 * z_far_mid + 1 - core)
            g_mates(n_line, 1)
            g_take(z_far_end, FROM_END, 8)
            g_take(z_far_mid, FROM_MID, 8)
            turn(acts, z_far_end)
            g_mates(n_line, 8)
            sum_block(8)
            turn(acts, z_far_mid)
            whole_block(0)
            whole_block(1)
            whole_block(2)
            whole_pair(3)
            whole_pair(5)
            whole_pair(7)
        else:
            act_send(2 * z_mid + 1 - core, mate, ends)
            spread(ends, me)
            act_send(mate, mate, acts)
            g_mine(4)
            g_mine(2)
            g_mine(0)
            pass_back(me, tp)
            for c in range(2):
                act_send(2 * z_far_end + c, 2 * z_far_mid + c, ends)
            spread(acts, me)
            piece(0)
            arrive(ends, mate)
            arrive(acts, mate)
            piece(1)
            part_one(0)
            piece(2)
            piece(3)
            piece(4)
            piece(5)
            relay(ends, me)
            piece(6)
            piece(7)
            relay(acts, me)
            g_take(z_mid, FROM_SIDE, 1)
            relay(ends, mate)
            arrive(acts, 2 * z_mid + core)
            part_one(1)
            relay(acts, mate)
            arrive(acts, 2 * z_mid + 1 - core)
            part_one(2)
            arrive(acts, 2 * z_far_mid + core)
            part_two(0)
            arrive(acts, 2 * z_far_mid + 1 - core)
            gathered(ends, z_end)
            pass_back(mate, next_)
            pass_back(mate, tp)
            g_mine(3)
            g_mine(5)
            g_mine(8)
            pass_back(me, next_)
            g_mine(6)
            g_mine(1)
            pass_back(me, diag)
            g_mine(7)
            pass_back(mate, near)
            pass_back(mate, diag)
            for c in range(2):
                act_send(2 * z_far_mid + c, 2 * z_far_mid + c, acts)
            pass_back(me, near)
            relay(acts, 2 * z_mid + core)
            part_one(3)
            g_take(z_mid, FROM_SIDE, 0)
            part_two(1)
            turn(acts, z_end)
            g_mates(1, 2)
            own_block(2)
            g_mates(1, 3)
            own_block(3)
            g_mates(1, 4)
            own_block(4)
            g_mates(1, 5)
            own_block(5)
            g_mates(1, 6)
            own_block(6)
            relay(acts, 2 * z_mid + 1 - core)
            g_mates(1, 7)
            own_block(7)
            g_mates(1, 8)
            own_block(8)
            g_take(z_far_mid, FROM_MID, 1)
            arrive(acts, 2 * z_far_end + core)
            part_two(2)
            part_sum(0)
            arrive(acts, 2 * z_far_end + 1 - core)
            relay(acts, 2 * z_far_mid + core)
            relay(acts, 2 * z_far_mid + 1 - core)
            part_one(4)
            part_one(5)
            part_one(6)
            g_take(z_far_end, FROM_END, 0)
            part_sum(1)
            part_one(7)
            part_two(3)
            turn(acts, z_mid)
            g_take(z_far_mid, FROM_MID, 0)
            relay(acts, 2 * z_far_end + core)
            g_mates(n_line, 0)
            relay(acts, 2 * z_far_end + 1 - core)
            part_sum(2)
            part_two(4)
            turn(acts, z_far_mid)
            part_two(5)
            part_sum(3)
            add_block(2)
            part_two(6)
            turn(acts, z_far_end)
            whole_block(0)
            part_sum(4)
            add_block(3)
            part_two(7)
            part_sum(5)
            part_sum(6)
            add_block(4)
            part_sum(7)
            add_block(5)
            add_block(6)
            add_block(7)
            g_take(z_far_end, FROM_END, 1)
            g_mates(n_line, 1)
            whole_block(1)
            add_block(8)
        all_sent()

    is_mid = z == z_mid

    @pl.when(is_mid)
    def _():
        program(True)

    @pl.when(jnp.logical_not(is_mid))
    def _():
        program(False)


def square_body(act_codes, scale_exps, weight, grad_out):
    n_ctx, n_tp = lax.axis_size("ctx"), lax.axis_size("tp")
    rows, width = act_codes.shape
    toks, cols = grad_out.shape
    feats = width // n_ctx
    d_tile = width // 8
    n_d = width // d_tile
    all_toks = toks * n_ctx
    n_b = len(blocks_of(cols))
    full = wide_blocks(cols)
    dma = pltpu.SemaphoreType.DMA
    vmem = pl.BlockSpec(memory_space=pltpu.VMEM)
    hbm = pl.BlockSpec(memory_space=pltpu.HBM)
    bf16 = jnp.bfloat16
    outs = rows * width * 2 + feats * cols * 4
    return pl.pallas_call(
        functools.partial(square_kernel, n_ctx, n_tp, all_toks),
        out_shape=(
            pltpu.VMEM((rows, width), bf16),
            pltpu.VMEM((feats, cols), jnp.float32),
        ),
        in_specs=[hbm, hbm, hbm, hbm],
        out_specs=(vmem, vmem),
        scratch_shapes=[
            pltpu.VMEM((rows, width), bf16),
            pltpu.VMEM(scale_exps.shape[::-1], scale_exps.dtype),
            pltpu.VMEM((n_d, d_tile, cols), bf16),
            pltpu.VMEM((toks, cols), bf16),
            pltpu.VMEM((full, all_toks, WIDE), bf16),
            pltpu.VMEM((n_b - full, all_toks, WIDE // 2), bf16),
            pltpu.VMEM((n_ctx, rows, feats), bf16),
            pltpu.VMEM((n_ctx, n_tp, rows, feats), bf16),
            pltpu.VMEM((n_ctx, n_tp, rows, feats), bf16),
            pltpu.VMEM((feats, all_toks), bf16),
            pltpu.VMEM((feats, all_toks - 2 * toks), bf16),
            pltpu.VMEM((n_d, n_tp, rows, d_tile), bf16),
            pltpu.VMEM((n_d, 2, rows, d_tile), bf16),
            pltpu.VMEM((n_d, rows, d_tile), bf16),
            pltpu.VMEM((n_d, rows, d_tile), bf16),
            pltpu.VMEM((max(full - RAW, 1), feats, WIDE), bf16),
            pltpu.VMEM((max(full - RAW, 1), feats, WIDE), bf16),
            pltpu.VMEM((n_b - full, feats, WIDE // 2), bf16),
            pltpu.VMEM((n_b - full, feats, WIDE // 2), bf16),
            dma((3,)),
            dma((2,)),
            dma((n_b,)),
            dma((11,)),
            dma((2, n_ctx)),
            dma((2, n_ctx)),
            dma((2, n_ctx // 2)),
            dma((3, n_b)),
            dma((n_b,)),
            dma((n_d,)),
            dma((n_d,)),
            dma((n_b,)),
        ],
        compiler_params=pltpu.CompilerParams(
            collective_id=0, has_side_effects=True, vmem_limit_bytes=67_043_328 - outs - 8192
        ),
    )(act_codes, scale_exps.T, weight, grad_out)


def body(act_codes, scale_exps, weight, grad_out):
    line, square = lax.axis_size("ctx") // 2, lax.axis_size("tp")
    if line == 4 and square == 4 and grad_out.shape[1] % WIDE == 0:
        return square_body(act_codes, scale_exps, weight, grad_out)
    return line_body(act_codes, scale_exps, weight, grad_out)


def solution(mesh):
    placed = (P(("ctx", "tp"), None), P(("ctx", "tp"), None), P(None, "tp"), P("ctx", "tp"))
    return jax.shard_map(
        body,
        mesh=mesh,
        in_specs=placed,
        out_specs=(P(("ctx", "tp"), None), P("ctx", "tp")),
        check_vma=False,
    )
```

```python
import functools
import math

import jax
import jax.numpy as jnp
from jax import lax
from jax.experimental import pallas as pl
from jax.experimental.pallas import tpu as pltpu
from jax.sharding import PartitionSpec as P

MESH = pl.DeviceIdType.MESH
CHUNKS = 4


def line_kernel(
    n_ctx, n_tp, tokens,
    codes_hbm, exps_hbm, weight_ref, grads_ref,
    gin_ref, gw_ref,
    codes_ref, exps_ref, w_buf, g_buf, a_send, a_buf, part, landed,
    in_sem, w_sem, g_sem,
    a_ssem, a_rsem, b_ssem, b_rsem, up_ssem, down_ssem, mate_ssem, g_rsem, p_ssem, p_rsem,
):
    n_line = n_ctx // 2
    me = lax.axis_index("ctx")
    tp = lax.axis_index("tp")
    core = lax.rem(me, 2)
    z = lax.div(me, 2)
    mate = me + 1 - 2 * core
    rows, width = codes_ref.shape
    block = width // exps_ref.shape[0]
    feats = width // n_ctx
    d_tile = w_buf.shape[1]
    n_d = w_buf.shape[0]
    scale = lax.rsqrt(jnp.float32(tokens))
    split = n_ctx * n_tp <= 64

    def load_w(i):
        return pltpu.make_async_copy(
            weight_ref.at[pl.ds(i * d_tile, d_tile)], w_buf.at[i], w_sem.at[i]
        )

    def load_g(k):
        size = g_buf.shape[2]
        return pltpu.make_async_copy(
            grads_ref.at[pl.ds(k * size, size)], g_buf.at[me, k], g_sem.at[k]
        )

    load_codes = pltpu.make_async_copy(codes_hbm, codes_ref, in_sem.at[0])
    load_exps = pltpu.make_async_copy(exps_hbm, exps_ref, in_sem.at[1])
    load_g(0).start()
    load_codes.start()
    load_exps.start()
    for k in range(1, CHUNKS):
        load_g(k).start()
    for i in range(n_d):
        load_w(i).start()

    barrier = pltpu.get_barrier_semaphore()
    for r in range(1, n_ctx):
        pl.semaphore_signal(
            barrier, inc=1, device_id=(lax.rem(me + r, n_ctx), tp), device_id_type=MESH
        )
    for r in range(1, n_tp):
        pl.semaphore_signal(
            barrier, inc=1, device_id=(me, lax.rem(tp + r, n_tp)), device_id_type=MESH
        )

    pl.semaphore_wait(barrier, n_ctx + n_tp - 2)

    def remote(src, dst, ssem, rsem, to):
        return pltpu.make_async_remote_copy(
            src_ref=src, dst_ref=dst, send_sem=ssem, recv_sem=rsem,
            device_id=to, device_id_type=MESH,
        )

    def act_copy(to):
        return remote(
            a_send.at[to], a_buf.at[me, tp], a_ssem.at[to], a_rsem.at[me], (to, tp)
        )

    def act_landing(source):
        return remote(
            a_send.at[source], a_buf.at[source, tp], a_ssem.at[source], a_rsem.at[source],
            (source, tp),
        )

    def spread_copy(s, q, src=None):
        return remote(
            a_buf.at[s, tp] if src is None else src,
            a_buf.at[s, tp], b_ssem.at[s, q], b_rsem.at[s, tp], (me, q),
        )

    def spread_landing(s, q):
        return remote(
            a_buf.at[s, q], a_buf.at[s, q], b_ssem.at[s, q], b_rsem.at[s, q], (me, q)
        )

    def spread_all(q):
        return remote(
            a_buf.at[:, tp], a_buf.at[:, tp], b_ssem.at[0, q], b_rsem.at[0, tp], (me, q)
        )

    def spread_all_landing(q):
        return remote(
            a_buf.at[:, q], a_buf.at[:, q], b_ssem.at[0, q], b_rsem.at[0, q], (me, q)
        )

    def pass_on(s, k, ssem, to):
        return remote(
            g_buf.at[s, k], g_buf.at[s, k], ssem.at[lax.div(s, 2), k], g_rsem.at[s, k], (to, tp)
        )

    def up(s, k):
        return pass_on(s, k, up_ssem, me + 2)

    def down(s, k):
        return pass_on(s, k, down_ssem, me - 2)

    def across(s, k):
        return pass_on(s, k, mate_ssem, mate)

    has_up = z < n_line - 1
    has_down = z > 0

    def send_own(k):
        load_g(k).wait()

        @pl.when(has_up)
        def _():
            up(me, k).start()

        @pl.when(has_down)
        def _():
            down(me, k).start()

        across(me, k).start()

    send_own(0)
    load_codes.wait()
    load_exps.wait()
    powers = jnp.exp2(exps_ref[...].astype(jnp.float32)).T
    for b in range(width // block):
        owner, place = divmod(b * block, feats)
        value = codes_ref[:, b * block : (b + 1) * block].astype(jnp.float32)
        value = value * powers[:, b : b + 1]
        a_send[owner, :, place : place + block] = value.astype(jnp.bfloat16)
    a_buf[me, tp] = a_send[me]
    for r in range(1, n_ctx):
        act_copy(lax.rem(me + r, n_ctx)).start()
    for k in range(1, CHUNKS):
        send_own(k)

    peers = [lax.rem(tp + r, n_tp) for r in range(1, n_tp)]
    if split:
        for q in peers:
            spread_copy(me, q, a_send.at[me]).start()

    grads = g_buf.at[me]

    def part_piece(i):
        load_w(i).wait()
        rows_all = grads[...].reshape(-1, g_buf.shape[3])
        piece = lax.dot_general(
            rows_all, w_buf[i], (((1,), (1,)), ((), ())), preferred_element_type=jnp.float32
        ).astype(jnp.bfloat16)
        part[:, :, i * d_tile : (i + 1) * d_tile] = piece.reshape(n_tp, rows, d_tile)

    per = -(-n_d // n_ctx)
    done = 0
    for r in range(1, n_ctx):
        for i in range(done, min(done + per, n_d)):
            part_piece(i)
        done = min(done + per, n_d)
        s = lax.rem(me - r + n_ctx, n_ctx)
        act_landing(s).wait_recv()
        if split:
            for q in peers:
                spread_copy(s, q).start()
    for i in range(done, n_d):
        part_piece(i)
    if not split:
        for q in peers:
            spread_all(q).start()

    def part_copy(q):
        return remote(part.at[q], landed.at[tp], p_ssem.at[q], p_rsem.at[tp], (me, q))

    def part_landing(q):
        return remote(part.at[q], landed.at[q], p_ssem.at[q], p_rsem.at[q], (me, q))

    for q in peers:
        part_copy(q).start()

    n_cols = g_buf.shape[3]
    n_tile = 512 if n_cols % 512 == 0 else n_cols

    def accumulate(zz, first, k=None):
        if k is None:
            lhs = a_buf[pl.ds(2 * zz, 2)].reshape(-1, feats).T
        else:
            size = n_tp // CHUNKS
            lhs = a_buf[pl.ds(2 * zz, 2), k * size : (k + 1) * size].reshape(-1, feats).T

        for j in range(n_cols // n_tile):
            cols = slice(j * n_tile, (j + 1) * n_tile)
            if k is None:
                rhs = g_buf[pl.ds(2 * zz, 2), :, :, cols].reshape(-1, n_tile)
            else:
                rhs = g_buf[pl.ds(2 * zz, 2), k, :, cols].reshape(-1, n_tile)
            term = jnp.dot(lhs, rhs, preferred_element_type=jnp.float32) * scale
            if first:
                gw_ref[:, cols] = term
            else:
                gw_ref[:, cols] += term

    def await_acts(zz, first):
        if split:
            for c in range(2):
                for q in peers:
                    spread_landing(2 * zz + c, q).wait_recv()
        elif first:
            for q in peers:
                spread_all_landing(q).wait_recv()

    def chip_terms(zz, first=False):
        other = 2 * zz + 1 - core
        for k in range(CHUNKS):
            across(other, k).wait_recv()
        await_acts(zz, first)
        accumulate(zz, first)

    def terms_at(d):
        if d == 0:
            chip_terms(z, True)
            return

        @pl.when(z >= d)
        def _():
            chip_terms(z - d)

        @pl.when(z + d < n_line)
        def _():
            chip_terms(z + d)

    def sum_parts():
        for q in peers:
            part_landing(q).wait_recv()
        total = part[tp].astype(jnp.float32)
        for q in peers:
            total = total + landed[q].astype(jnp.float32)
        gin_ref[...] = total.astype(jnp.bfloat16)

    def from_below(d, k):
        s = me - 2 * d
        up(s, k).wait_recv()

        @pl.when(has_up)
        def _():
            up(s, k).start()

        across(s, k).start()

    def from_above(d, k):
        s = me + 2 * d
        down(s, k).wait_recv()

        @pl.when(has_down)
        def _():
            down(s, k).start()

        across(s, k).start()

    for d in range(1, n_line - 1):
        for k in range(CHUNKS):

            @pl.when(z >= d)
            def _():
                from_below(d, k)

            @pl.when(z + d < n_line)
            def _():
                from_above(d, k)

        terms_at(d - 1)

    d = n_line - 1
    terms_at(d - 1)

    def last_terms(zz, arrive):
        other = 2 * zz + 1 - core
        await_acts(zz, False)
        for k in range(CHUNKS):
            arrive(d, k)
            if k == CHUNKS - 1:
                sum_parts()
            if k > 0:
                across(other, k - 1).wait_recv()
                accumulate(zz, False, k - 1)
        across(other, CHUNKS - 1).wait_recv()
        accumulate(zz, False, CHUNKS - 1)

    @pl.when(z == d)
    def _():
        last_terms(0, from_below)

    @pl.when(z == 0)
    def _():
        last_terms(d, from_above)

    @pl.when((z > 0) & (z < d))
    def _():
        sum_parts()

    for r in range(1, n_ctx):
        act_copy(lax.rem(me + r, n_ctx)).wait_send()
    for q in peers:
        part_copy(q).wait_send()
        if split:
            for s in range(n_ctx):
                spread_copy(s, q).wait_send()
        else:
            spread_all(q).wait_send()
    for zz in range(n_line):
        for k in range(CHUNKS):
            s = 2 * zz + core
            across(s, k).wait_send()

            @pl.when(has_up & (zz <= z))
            def _():
                up(s, k).wait_send()

            @pl.when(has_down & (zz >= z))
            def _():
                down(s, k).wait_send()


def line_body(act_codes, scale_exps, weight, grad_out):
    n_ctx, n_tp = lax.axis_size("ctx"), lax.axis_size("tp")
    n_line = n_ctx // 2
    rows, width = act_codes.shape
    toks, cols = grad_out.shape
    feats = width // n_ctx
    d_tile = min(512, width)
    dma = pltpu.SemaphoreType.DMA
    lanes = -(-cols // 128) * 128
    outs = -(-rows // 16) * 16 * width * 2 + feats * lanes * 4
    vmem = pl.BlockSpec(memory_space=pltpu.VMEM)
    hbm = pl.BlockSpec(memory_space=pltpu.HBM)
    bf16 = jnp.bfloat16
    return pl.pallas_call(
        functools.partial(line_kernel, n_ctx, n_tp, toks * n_ctx),
        out_shape=(
            pltpu.VMEM((rows, width), bf16),
            pltpu.VMEM((feats, cols), jnp.float32),
        ),
        in_specs=[hbm, hbm, hbm, hbm],
        out_specs=(vmem, vmem),
        scratch_shapes=[
            pltpu.VMEM((rows, width), bf16),
            pltpu.VMEM(scale_exps.shape[::-1], scale_exps.dtype),
            pltpu.VMEM((width // d_tile, d_tile, cols), bf16),
            pltpu.VMEM((n_ctx, CHUNKS, toks // CHUNKS, cols), bf16),
            pltpu.VMEM((n_ctx, rows, feats), bf16),
            pltpu.VMEM((n_ctx, n_tp, rows, feats), bf16),
            pltpu.VMEM((n_tp, rows, width), bf16),
            pltpu.VMEM((n_tp, rows, width), bf16),
            dma((2,)),
            dma((width // d_tile,)),
            dma((CHUNKS,)),
            dma((n_ctx,)),
            dma((n_ctx,)),
            dma((n_ctx if n_ctx * n_tp <= 64 else 1, n_tp)),
            dma((n_ctx if n_ctx * n_tp <= 64 else 1, n_tp)),
            dma((n_line, CHUNKS)),
            dma((n_line, CHUNKS)),
            dma((n_line, CHUNKS)),
            dma((n_ctx, CHUNKS)),
            dma((n_tp,)),
            dma((n_tp,)),
        ],
        compiler_params=pltpu.CompilerParams(
            collective_id=0, has_side_effects=True, vmem_limit_bytes=67_043_328 - outs - 8192
        ),
    )(act_codes, scale_exps.T, weight, grad_out)


RAW = 1
WIDE = 256


def wide_blocks(cols):
    return cols // WIDE * 3 // 6


def blocks_of(cols):
    full = wide_blocks(cols)
    slim = WIDE // 2
    return [(b * WIDE, WIDE) for b in range(full)] + [
        (start, slim) for start in range(full * WIDE, cols, slim)
    ]


def square_kernel(
    n_ctx, n_tp, tokens,
    codes_hbm, exps_hbm, weight_ref, grads_ref,
    gin_ref, gw_ref,
    codes_ref, exps_ref, w_buf, g_own, g_wide, g_slim, a_send, a_buf, p_buf, a_t, p_t,
    part, recv1, total1, recv2, sums_out, sums_in, slim_out, slim_in,
    in_sem, w_sem, s_sem, line_sem, near_sem, rest_sem, g_rsem, mate_sem,
    one_sem, two_sem, sum_sem,
):
    me = lax.axis_index("ctx")
    tp = lax.axis_index("tp")
    core = lax.rem(me, 2)
    z = lax.div(me, 2)
    mate = me + 1 - 2 * core
    n_line = n_ctx // 2
    side = lax.div(z, 2)
    z_end, z_mid = (n_line - 1) * side, 1 + side
    z_far_mid, z_far_end = 2 - side, (n_line - 1) * (1 - side)
    y, x = lax.div(tp, 2), lax.rem(tp, 2)
    by_x, by_y = 2 * y + 1 - x, 2 * (1 - y) + x
    near = by_x + core * (by_y - by_x)
    next_ = by_y + core * (by_x - by_y)
    diag = n_tp - 1 - tp
    rows, width = codes_ref.shape
    toks = g_own.shape[0]
    block = width // exps_ref.shape[0]
    feats = width // n_ctx
    d_tile = w_buf.shape[1]
    n_d = w_buf.shape[0]
    chip = 2 * toks
    unit = rows * feats
    scale = lax.rsqrt(jnp.float32(tokens))
    blocks = blocks_of(g_own.shape[1])
    n_b = len(blocks)
    full = g_wide.shape[0]

    def g_at(b):
        return g_wide.at[b] if b < full else g_slim.at[b - full]

    def g_piece(s, b):
        return g_at(b).at[pl.ds(s * toks, toks)]

    def load_w(i):
        return pltpu.make_async_copy(
            weight_ref.at[pl.ds(i * d_tile, d_tile)], w_buf.at[i], w_sem.at[i % 2]
        )

    def load_g(b):
        start, size = blocks[b]
        return pltpu.make_async_copy(
            grads_ref.at[:, pl.ds(start, size)], g_piece(me, b), in_sem.at[3]
        )

    load_codes = pltpu.make_async_copy(codes_hbm, codes_ref, in_sem.at[0])
    load_exps = pltpu.make_async_copy(exps_hbm, exps_ref, in_sem.at[1])
    load_own = pltpu.make_async_copy(grads_ref, g_own, in_sem.at[2])
    load_codes.start()
    load_exps.start()
    for b in range(n_b):
        load_g(b).start()

    barrier = pltpu.get_barrier_semaphore()
    for r in range(1, n_ctx):
        pl.semaphore_signal(
            barrier, inc=1, device_id=(lax.rem(me + r, n_ctx), tp), device_id_type=MESH
        )
    for r in range(1, n_tp):
        pl.semaphore_signal(
            barrier, inc=1, device_id=(me, lax.rem(tp + r, n_tp)), device_id_type=MESH
        )
    load_exps.wait()
    load_codes.wait()
    load_w(0).start()
    load_w(1).start()
    powers = jnp.exp2(exps_ref[...].astype(jnp.float32)).T
    for b in range(width // block):
        owner, place = divmod(b * block, feats)
        value = codes_ref[:, b * block : (b + 1) * block].astype(jnp.float32)
        value = value * powers[:, b : b + 1]
        a_send[owner, :, place : place + block] = value.astype(jnp.bfloat16)
    a_buf[me, tp] = a_send[me]
    p_buf[me, tp] = a_send[2 * (z_mid + z_end - z) + core]
    pltpu.make_async_copy(grads_ref, g_own, in_sem.at[3]).wait()
    load_own.start()
    pl.semaphore_wait(barrier, n_ctx + n_tp - 2)

    def program(is_mid):
        sent = {}

        def remote(src, dst, ssem, rsem, to):
            return pltpu.make_async_remote_copy(
                src_ref=src, dst_ref=dst, send_sem=ssem, recv_sem=rsem,
                device_id=to, device_id_type=MESH,
            )

        def send(kind, src, dst, rsem, to):
            remote(src, dst, s_sem.at[kind], rsem, to).start()
            sent[kind] = sent.get(kind, 0) + math.prod(src.shape) // unit

        def landed(dst, rsem):
            remote(dst, dst, s_sem.at[0], rsem, (me, tp)).wait_recv()

        def all_sent():
            for kind, n in sent.items():
                if n % 24 == 0:
                    ref = w_buf.at[pl.ds(0, n // 24)]
                elif n % 2 == 0 and n // 2 <= n_d:
                    ref = recv1.at[pl.ds(0, n // 2)]
                elif n <= n_d:
                    ref = recv2.at[pl.ds(0, n)]
                elif n % 3 == 0 and n // 3 <= n_d:
                    ref = part.at[pl.ds(0, n // 3), pl.ds(0, 3)]
                else:
                    ref = a_buf.at[pl.ds(0, n // n_tp)]
                assert math.prod(ref.shape) == n * unit
                remote(ref, ref, s_sem.at[kind], near_sem.at[0, 0], (me, tp)).wait_send()

        def both(zz):
            return (2 * zz, 2 * zz + 1)

        acts, ends = (a_buf, 0), (p_buf, 1)

        def act_send(d, to, kind):
            buf, k = kind
            send(0, a_send.at[d], buf.at[me, tp], line_sem.at[k, me], (to, tp))

        def spread(kind, s):
            buf, k = kind
            send(1, buf.at[s, tp], buf.at[s, tp], near_sem.at[k, s], (me, near))
            send(2, buf.at[s, tp], buf.at[s, tp], rest_sem.at[k, lax.div(s, 2)], (me, next_))

        def pass_end(s):
            send(3, p_buf.at[s, tp], a_buf.at[s, tp], line_sem.at[0, s], (2 * z_end + core, tp))

        def arrive(kind, s):
            buf, k = kind
            landed(buf.at[s, tp], line_sem.at[k, s])
            spread(kind, s)
            if k == 1 and is_mid:
                pass_end(s)

        def relay(kind, s):
            buf, k = kind
            landed(buf.at[s, near], near_sem.at[k, s])
            send(4, buf.at[s, near], buf.at[s, near], rest_sem.at[k, lax.div(s, 2)], (me, next_))

        def gathered(kind, zz):
            buf, k = kind
            landed(buf.at[2 * zz], rest_sem.at[k, zz])

        def pass_back(s, q):
            send(
                3, p_buf.at[s, q], a_buf.at[s, q], rest_sem.at[0, lax.div(s, 2)],
                (2 * z_mid + core, tp),
            )

        def turned(kind, zz):
            buf, k = kind
            value = buf[pl.ds(2 * zz, 2)].reshape(chip, feats).T
            if k == 0:
                a_t[:, pl.ds(pl.multiple_of(zz * chip, chip), chip)] = value
            else:
                p_t[:, pl.ds(pl.multiple_of((zz - 1 + side) * chip, chip), chip)] = value

        def turn(kind, zz):
            gathered(kind, zz)
            turned(kind, zz)

        def turn_whole(zz):
            landed(a_buf.at[pl.ds(2 * zz, 2)], rest_sem.at[0, zz])
            turned(acts, zz)

        def g_send(kind, s, b, rsem, to):
            send(kind, g_piece(s, b), g_piece(s, b), rsem, (to, tp))

        inward = 2 * (z_far_mid if is_mid else z_mid) + core
        outward = 2 * z_end + core
        FROM_SIDE, FROM_MID, FROM_END = 0, 1, 2

        def g_mine(b):
            g_send(5, me, b, g_rsem.at[FROM_MID if is_mid else FROM_SIDE, b], inward)
            if is_mid and b < RAW:
                g_send(6, me, b, g_rsem.at[FROM_SIDE, b], outward)
            g_send(7, me, b, mate_sem.at[b], mate)

        def g_take(zz, way, b):
            s = 2 * zz + core
            landed(g_piece(s, b), g_rsem.at[way, b])
            if is_mid and way == FROM_SIDE:
                g_send(5, s, b, g_rsem.at[FROM_END, b], inward)
            elif is_mid and b < RAW:
                g_send(6, s, b, g_rsem.at[way, b], outward)
            g_send(7, s, b, mate_sem.at[b], mate)

        def g_mates(n, b):
            landed(g_at(b).at[pl.ds(0, n * toks)], mate_sem.at[b])

        def piece(i):
            if i == 0:
                load_own.wait()
            load_w(i).wait()
            if i + 2 < n_d:
                load_w(i + 2).start()
            value = lax.dot_general(
                g_own[...], w_buf[i], (((1,), (1,)), ((), ())), preferred_element_type=jnp.float32
            ).astype(jnp.bfloat16)
            value = value.reshape(n_tp, rows, d_tile)
            for q in range(n_tp):
                dy, dx = lax.rem(y + q // 2, 2), lax.rem(x + q % 2, 2)
                slot = 2 * dx + dy + core * (dy - dx)
                part[i, slot] = value[q]

        def part_one(i):
            send(8, part.at[i, pl.ds(2, 2)], recv1.at[i], one_sem.at[i], (me, near))

        def part_two(i):
            landed(recv1.at[i], one_sem.at[i])
            total = part[i, 1].astype(jnp.float32) + recv1[i, 1].astype(jnp.float32)
            total1[i] = total.astype(jnp.bfloat16)
            send(9, total1.at[i], recv2.at[i], two_sem.at[i], (me, next_))

        def part_sum(i):
            landed(recv2.at[i], two_sem.at[i])
            total = part[i, 0].astype(jnp.float32) + recv1[i, 0].astype(jnp.float32)
            total = total + recv2[i].astype(jnp.float32)
            gin_ref[:, i * d_tile : (i + 1) * d_tile] = total.astype(jnp.bfloat16)

        def dot(lhs, rhs):
            return jnp.dot(lhs, rhs, preferred_element_type=jnp.float32)

        halves = [slice(h * (feats // 2), (h + 1) * (feats // 2)) for h in range(2)]

        def cols(b):
            start, size = blocks[b]
            return slice(start, start + size)

        def whole_block(b):
            for half in halves:
                gw_ref[half, cols(b)] = dot(a_t[half], g_at(b)[...]) * scale

        def whole_pair(b):
            start, size = blocks[b]
            for half in halves:
                rhs = jnp.concatenate([g_at(b)[...], g_at(b + 1)[...]], axis=1)
                gw_ref[half, start : start + 2 * size] = dot(a_t[half], rhs) * scale

        def out_at(b):
            return sums_out.at[b - RAW] if b < full else slim_out.at[b - full]

        def in_at(b):
            return sums_in.at[b - RAW] if b < full else slim_in.at[b - full]

        def sum_block(b):
            first = pl.multiple_of((1 - side) * chip, chip)
            for half in halves:
                rhs = g_at(b)[pl.ds(first, (n_line - 1) * chip)]
                out_at(b)[half] = dot(p_t[half], rhs).astype(jnp.bfloat16)
                send(10, out_at(b).at[half], in_at(b).at[half], sum_sem.at[b - RAW], (outward, tp))

        def own_block(b):
            here = pl.ds(pl.multiple_of(z_end * chip, chip), chip)
            for half in halves:
                gw_ref[half, cols(b)] = dot(a_t[half, here], g_at(b)[here])

        def add_block(b):
            landed(in_at(b), sum_sem.at[b - RAW])
            gw_ref[:, cols(b)] = (gw_ref[:, cols(b)] + in_at(b)[...].astype(jnp.float32)) * scale

        if is_mid:
            for c in range(2):
                act_send(2 * z_far_end + c, 2 * z_far_mid + c, ends)
            g_mine(1)
            g_mine(0)
            g_mine(3)
            pass_end(me)
            act_send(2 * z_end + 1 - core, mate, ends)
            spread(ends, me)
            spread(acts, me)
            act_send(mate, mate, acts)
            piece(0)
            piece(1)
            arrive(ends, mate)
            arrive(acts, mate)
            piece(2)
            piece(3)
            piece(4)
            arrive(ends, 2 * z_far_mid + core)
            piece(5)
            piece(6)
            relay(ends, me)
            arrive(ends, 2 * z_far_mid + 1 - core)
            g_take(z_end, FROM_SIDE, 1)
            piece(7)
            relay(acts, me)
            relay(ends, mate)
            arrive(ends, 2 * z_far_end + core)
            relay(acts, mate)
            relay(ends, 2 * z_far_mid + core)
            g_take(z_far_mid, FROM_MID, 1)
            arrive(ends, 2 * z_far_end + 1 - core)
            relay(ends, 2 * z_far_mid + 1 - core)
            relay(ends, 2 * z_far_end + core)
            g_take(z_far_mid, FROM_MID, 0)
            g_take(z_far_mid, FROM_MID, 3)
            turn(ends, z_mid)
            g_take(z_end, FROM_SIDE, 0)
            part_one(0)
            relay(ends, 2 * z_far_end + 1 - core)
            turn(acts, z_mid)
            g_take(z_far_end, FROM_END, 1)
            g_take(z_end, FROM_SIDE, 2)
            g_mine(2)
            g_mates(n_line, 1)
            part_one(1)
            turn(ends, z_far_mid)
            g_take(z_far_end, FROM_END, 0)
            part_two(0)
            turn(ends, z_far_end)
            g_mates(n_line, 0)
            g_take(z_end, FROM_SIDE, 3)
            for c in range(2):
                act_send(2 * z_far_mid + c, 2 * z_far_mid + c, acts)
            sum_block(1)
            g_take(z_far_end, FROM_END, 2)
            part_two(1)
            g_take(z_far_mid, FROM_MID, 2)
            g_take(z_end, FROM_SIDE, 4)
            g_mine(4)
            g_mine(5)
            g_take(z_end, FROM_SIDE, 5)
            g_mine(6)
            part_one(2)
            part_one(3)
            g_mates(n_line, 2)
            sum_block(2)
            g_take(z_far_end, FROM_END, 3)
            part_one(4)
            part_one(5)
            g_mates(n_line, 3)
            sum_block(3)
            arrive(acts, 2 * z_far_mid + core)
            arrive(acts, 2 * z_far_end + core)
            part_two(2)
            part_two(3)
            arrive(acts, 2 * z_far_mid + 1 - core)
            arrive(acts, 2 * z_far_end + 1 - core)
            g_take(z_far_end, FROM_END, 4)
            g_take(z_end, FROM_SIDE, 6)
            g_mine(7)
            g_take(z_end, FROM_SIDE, 7)
            g_mine(8)
            g_take(z_end, FROM_SIDE, 8)
            part_two(4)
            part_one(6)
            part_one(7)
            g_take(z_far_mid, FROM_MID, 4)
            g_mates(n_line, 4)
            sum_block(4)
            g_take(z_far_mid, FROM_MID, 5)
            part_two(5)
            g_take(z_far_end, FROM_END, 5)
            relay(acts, 2 * z_far_mid + core)
            g_mates(n_line, 5)
            sum_block(5)
            g_take(z_far_mid, FROM_MID, 6)
            relay(acts, 2 * z_far_end + core)
            g_take(z_far_end, FROM_END, 6)
            turn_whole(z_end)
            relay(acts, 2 * z_far_mid + 1 - core)
            g_mates(n_line, 6)
            sum_block(6)
            g_take(z_far_mid, FROM_MID, 7)
            relay(acts, 2 * z_far_end + 1 - core)
            g_take(z_far_end, FROM_END, 7)
            g_mates(n_line, 7)
            sum_block(7)
            g_take(z_far_mid, FROM_MID, 8)
            part_two(6)
            g_take(z_far_end, FROM_END, 8)
            g_mates(n_line, 8)
            sum_block(8)
            part_two(7)
            turn(acts, z_far_mid)
            turn(acts, z_far_end)
            whole_block(0)
            whole_block(1)
            whole_block(2)
            whole_pair(3)
            whole_pair(5)
            whole_pair(7)
            part_sum(0)
            part_sum(1)
            part_sum(2)
            part_sum(3)
            part_sum(4)
            part_sum(5)
            part_sum(6)
            part_sum(7)
        else:
            act_send(2 * z_mid + 1 - core, mate, ends)
            spread(ends, me)
            act_send(mate, mate, acts)
            g_mine(1)
            for c in range(2):
                act_send(2 * z_far_end + c, 2 * z_far_mid + c, ends)
            pass_back(me, tp)
            g_mine(0)
            g_mine(2)
            spread(acts, me)
            piece(0)
            piece(1)
            arrive(ends, mate)
            arrive(acts, mate)
            part_one(0)
            piece(2)
            piece(3)
            piece(4)
            piece(5)
            piece(6)
            relay(ends, me)
            g_take(z_mid, FROM_SIDE, 0)
            piece(7)
            part_one(1)
            relay(acts, me)
            part_one(2)
            arrive(acts, 2 * z_mid + core)
            relay(ends, mate)
            arrive(acts, 2 * z_mid + 1 - core)
            part_one(3)
            relay(acts, mate)
            arrive(acts, 2 * z_far_mid + core)
            arrive(acts, 2 * z_far_mid + 1 - core)
            part_one(4)
            part_one(5)
            part_two(0)
            arrive(acts, 2 * z_far_end + core)
            part_one(6)
            gathered(ends, z_end)
            pass_back(me, diag)
            g_mine(7)
            g_mine(3)
            g_mine(5)
            g_mine(8)
            g_mine(4)
            pass_back(me, near)
            for c in range(2):
                act_send(2 * z_far_mid + c, 2 * z_far_mid + c, acts)
            g_mine(6)
            pass_back(mate, near)
            pass_back(me, next_)
            pass_back(mate, diag)
            pass_back(mate, next_)
            pass_back(mate, tp)
            arrive(acts, 2 * z_far_end + 1 - core)
            part_two(1)
            part_one(7)
            turn(acts, z_end)
            g_mates(1, 1)
            own_block(1)
            g_mates(1, 2)
            own_block(2)
            g_mates(1, 3)
            own_block(3)
            g_take(z_far_mid, FROM_MID, 0)
            g_mates(1, 4)
            own_block(4)
            g_mates(1, 5)
            own_block(5)
            relay(acts, 2 * z_mid + core)
            g_mates(1, 6)
            own_block(6)
            g_mates(1, 7)
            own_block(7)
            g_mates(1, 8)
            own_block(8)
            part_two(2)
            relay(acts, 2 * z_mid + 1 - core)
            part_sum(0)
            part_two(3)
            relay(acts, 2 * z_far_mid + core)
            g_take(z_far_end, FROM_END, 0)
            relay(acts, 2 * z_far_mid + 1 - core)
            part_sum(1)
            g_mates(n_line, 0)
            part_sum(2)
            part_two(4)
            turn(acts, z_mid)
            add_block(1)
            part_sum(3)
            part_two(5)
            relay(acts, 2 * z_far_end + core)
            turn(acts, z_far_mid)
            part_sum(4)
            part_two(6)
            add_block(2)
            relay(acts, 2 * z_far_end + 1 - core)
            part_sum(5)
            add_block(3)
            part_two(7)
            part_sum(6)
            turn(acts, z_far_end)
            whole_block(0)
            add_block(4)
            part_sum(7)
            add_block(5)
            add_block(6)
            add_block(7)
            add_block(8)
        all_sent()

    is_mid = z == z_mid

    @pl.when(is_mid)
    def _():
        program(True)

    @pl.when(jnp.logical_not(is_mid))
    def _():
        program(False)


def square_body(act_codes, scale_exps, weight, grad_out):
    n_ctx, n_tp = lax.axis_size("ctx"), lax.axis_size("tp")
    rows, width = act_codes.shape
    toks, cols = grad_out.shape
    feats = width // n_ctx
    d_tile = width // 8
    n_d = width // d_tile
    all_toks = toks * n_ctx
    n_b = len(blocks_of(cols))
    full = wide_blocks(cols)
    dma = pltpu.SemaphoreType.DMA
    vmem = pl.BlockSpec(memory_space=pltpu.VMEM)
    hbm = pl.BlockSpec(memory_space=pltpu.HBM)
    bf16 = jnp.bfloat16
    outs = rows * width * 2 + feats * cols * 4
    gin, gw = pl.pallas_call(
        functools.partial(square_kernel, n_ctx, n_tp, all_toks),
        out_shape=(
            pltpu.VMEM((rows, width), bf16),
            pltpu.VMEM((feats, cols), jnp.float32),
        ),
        in_specs=[hbm, hbm, hbm, hbm],
        out_specs=(vmem, vmem),
        scratch_shapes=[
            pltpu.VMEM((rows, width), bf16),
            pltpu.VMEM(scale_exps.shape[::-1], scale_exps.dtype),
            pltpu.VMEM((n_d, d_tile, cols), bf16),
            pltpu.VMEM((toks, cols), bf16),
            pltpu.VMEM((full, all_toks, WIDE), bf16),
            pltpu.VMEM((n_b - full, all_toks, WIDE // 2), bf16),
            pltpu.VMEM((n_ctx, rows, feats), bf16),
            pltpu.VMEM((n_ctx, n_tp, rows, feats), bf16),
            pltpu.VMEM((n_ctx, n_tp, rows, feats), bf16),
            pltpu.VMEM((feats, all_toks), bf16),
            pltpu.VMEM((feats, all_toks - 2 * toks), bf16),
            pltpu.VMEM((n_d, n_tp, rows, d_tile), bf16),
            pltpu.VMEM((n_d, 2, rows, d_tile), bf16),
            pltpu.VMEM((n_d, rows, d_tile), bf16),
            pltpu.VMEM((n_d, rows, d_tile), bf16),
            pltpu.VMEM((max(full - RAW, 1), feats, WIDE), bf16),
            pltpu.VMEM((max(full - RAW, 1), feats, WIDE), bf16),
            pltpu.VMEM((n_b - full, feats, WIDE // 2), bf16),
            pltpu.VMEM((n_b - full, feats, WIDE // 2), bf16),
            dma((4,)),
            dma((2,)),
            dma((11,)),
            dma((2, n_ctx)),
            dma((2, n_ctx)),
            dma((2, n_ctx // 2)),
            dma((3, n_b)),
            dma((n_b,)),
            dma((n_d,)),
            dma((n_d,)),
            dma((n_b - RAW,)),
        ],
        compiler_params=pltpu.CompilerParams(
            collective_id=0, has_side_effects=True, vmem_limit_bytes=67_043_328 - outs - 8192
        ),
    )(act_codes, scale_exps.T, weight, grad_out)
    return pl.pallas_call(
        store_kernel,
        out_shape=(
            jax.ShapeDtypeStruct(gin.shape, gin.dtype), jax.ShapeDtypeStruct(gw.shape, gw.dtype)
        ),
        in_specs=[vmem, vmem],
        out_specs=(hbm, hbm),
        scratch_shapes=[dma((2,))],
        compiler_params=pltpu.CompilerParams(vmem_limit_bytes=1 << 20),
    )(gin, gw)


def store_kernel(gin_ref, gw_ref, gin_out, gw_out, sem):
    copies = [
        pltpu.make_async_copy(gw_ref, gw_out, sem.at[0]),
        pltpu.make_async_copy(gin_ref, gin_out, sem.at[1]),
    ]
    for copy in copies:
        copy.start()
    for copy in copies:
        copy.wait()


def body(act_codes, scale_exps, weight, grad_out):
    line, square = lax.axis_size("ctx") // 2, lax.axis_size("tp")
    if line == 4 and square == 4 and grad_out.shape[1] % WIDE == 0:
        return square_body(act_codes, scale_exps, weight, grad_out)
    return line_body(act_codes, scale_exps, weight, grad_out)


def solution(mesh):
    placed = (P(("ctx", "tp"), None), P(("ctx", "tp"), None), P(None, "tp"), P("ctx", "tp"))
    return jax.shard_map(
        body,
        mesh=mesh,
        in_specs=placed,
        out_specs=(P(("ctx", "tp"), None), P("ctx", "tp")),
        check_vma=False,
    )
```

```python
import functools
import math

import jax
import jax.numpy as jnp
from jax import lax
from jax.experimental import pallas as pl
from jax.experimental.pallas import tpu as pltpu
from jax.sharding import PartitionSpec as P

MESH = pl.DeviceIdType.MESH
CHUNKS = 4


def line_kernel(
    n_ctx, n_tp, tokens,
    codes_hbm, exps_hbm, weight_ref, grads_ref,
    gin_ref, gw_ref,
    codes_ref, exps_ref, w_buf, g_buf, a_send, a_buf, part, landed,
    in_sem, w_sem, g_sem,
    a_ssem, a_rsem, b_ssem, b_rsem, up_ssem, down_ssem, mate_ssem, g_rsem, p_ssem, p_rsem,
):
    n_line = n_ctx // 2
    me = lax.axis_index("ctx")
    tp = lax.axis_index("tp")
    core = lax.rem(me, 2)
    z = lax.div(me, 2)
    mate = me + 1 - 2 * core
    rows, width = codes_ref.shape
    block = width // exps_ref.shape[0]
    feats = width // n_ctx
    d_tile = w_buf.shape[1]
    n_d = w_buf.shape[0]
    scale = lax.rsqrt(jnp.float32(tokens))
    split = n_ctx * n_tp <= 64

    def load_w(i):
        return pltpu.make_async_copy(
            weight_ref.at[pl.ds(i * d_tile, d_tile)], w_buf.at[i], w_sem.at[i]
        )

    def load_g(k):
        size = g_buf.shape[2]
        return pltpu.make_async_copy(
            grads_ref.at[pl.ds(k * size, size)], g_buf.at[me, k], g_sem.at[k]
        )

    load_codes = pltpu.make_async_copy(codes_hbm, codes_ref, in_sem.at[0])
    load_exps = pltpu.make_async_copy(exps_hbm, exps_ref, in_sem.at[1])
    load_g(0).start()
    load_codes.start()
    load_exps.start()
    for k in range(1, CHUNKS):
        load_g(k).start()
    for i in range(n_d):
        load_w(i).start()

    barrier = pltpu.get_barrier_semaphore()
    for r in range(1, n_ctx):
        pl.semaphore_signal(
            barrier, inc=1, device_id=(lax.rem(me + r, n_ctx), tp), device_id_type=MESH
        )
    for r in range(1, n_tp):
        pl.semaphore_signal(
            barrier, inc=1, device_id=(me, lax.rem(tp + r, n_tp)), device_id_type=MESH
        )

    pl.semaphore_wait(barrier, n_ctx + n_tp - 2)

    def remote(src, dst, ssem, rsem, to):
        return pltpu.make_async_remote_copy(
            src_ref=src, dst_ref=dst, send_sem=ssem, recv_sem=rsem,
            device_id=to, device_id_type=MESH,
        )

    def act_copy(to):
        return remote(
            a_send.at[to], a_buf.at[me, tp], a_ssem.at[to], a_rsem.at[me], (to, tp)
        )

    def act_landing(source):
        return remote(
            a_send.at[source], a_buf.at[source, tp], a_ssem.at[source], a_rsem.at[source],
            (source, tp),
        )

    def spread_copy(s, q, src=None):
        return remote(
            a_buf.at[s, tp] if src is None else src,
            a_buf.at[s, tp], b_ssem.at[s, q], b_rsem.at[s, tp], (me, q),
        )

    def spread_landing(s, q):
        return remote(
            a_buf.at[s, q], a_buf.at[s, q], b_ssem.at[s, q], b_rsem.at[s, q], (me, q)
        )

    def spread_all(q):
        return remote(
            a_buf.at[:, tp], a_buf.at[:, tp], b_ssem.at[0, q], b_rsem.at[0, tp], (me, q)
        )

    def spread_all_landing(q):
        return remote(
            a_buf.at[:, q], a_buf.at[:, q], b_ssem.at[0, q], b_rsem.at[0, q], (me, q)
        )

    def pass_on(s, k, ssem, to):
        return remote(
            g_buf.at[s, k], g_buf.at[s, k], ssem.at[lax.div(s, 2), k], g_rsem.at[s, k], (to, tp)
        )

    def up(s, k):
        return pass_on(s, k, up_ssem, me + 2)

    def down(s, k):
        return pass_on(s, k, down_ssem, me - 2)

    def across(s, k):
        return pass_on(s, k, mate_ssem, mate)

    has_up = z < n_line - 1
    has_down = z > 0

    def send_own(k):
        load_g(k).wait()

        @pl.when(has_up)
        def _():
            up(me, k).start()

        @pl.when(has_down)
        def _():
            down(me, k).start()

        across(me, k).start()

    send_own(0)
    load_codes.wait()
    load_exps.wait()
    powers = jnp.exp2(exps_ref[...].astype(jnp.float32)).T
    for b in range(width // block):
        owner, place = divmod(b * block, feats)
        value = codes_ref[:, b * block : (b + 1) * block].astype(jnp.float32)
        value = value * powers[:, b : b + 1]
        a_send[owner, :, place : place + block] = value.astype(jnp.bfloat16)
    a_buf[me, tp] = a_send[me]
    for r in range(1, n_ctx):
        act_copy(lax.rem(me + r, n_ctx)).start()
    for k in range(1, CHUNKS):
        send_own(k)

    peers = [lax.rem(tp + r, n_tp) for r in range(1, n_tp)]
    if split:
        for q in peers:
            spread_copy(me, q, a_send.at[me]).start()

    grads = g_buf.at[me]

    def part_piece(i):
        load_w(i).wait()
        rows_all = grads[...].reshape(-1, g_buf.shape[3])
        piece = lax.dot_general(
            rows_all, w_buf[i], (((1,), (1,)), ((), ())), preferred_element_type=jnp.float32
        ).astype(jnp.bfloat16)
        part[:, :, i * d_tile : (i + 1) * d_tile] = piece.reshape(n_tp, rows, d_tile)

    per = -(-n_d // n_ctx)
    done = 0
    for r in range(1, n_ctx):
        for i in range(done, min(done + per, n_d)):
            part_piece(i)
        done = min(done + per, n_d)
        s = lax.rem(me - r + n_ctx, n_ctx)
        act_landing(s).wait_recv()
        if split:
            for q in peers:
                spread_copy(s, q).start()
    for i in range(done, n_d):
        part_piece(i)
    if not split:
        for q in peers:
            spread_all(q).start()

    def part_copy(q):
        return remote(part.at[q], landed.at[tp], p_ssem.at[q], p_rsem.at[tp], (me, q))

    def part_landing(q):
        return remote(part.at[q], landed.at[q], p_ssem.at[q], p_rsem.at[q], (me, q))

    for q in peers:
        part_copy(q).start()

    n_cols = g_buf.shape[3]
    n_tile = 512 if n_cols % 512 == 0 else n_cols

    def accumulate(zz, first, k=None):
        if k is None:
            lhs = a_buf[pl.ds(2 * zz, 2)].reshape(-1, feats).T
        else:
            size = n_tp // CHUNKS
            lhs = a_buf[pl.ds(2 * zz, 2), k * size : (k + 1) * size].reshape(-1, feats).T

        for j in range(n_cols // n_tile):
            cols = slice(j * n_tile, (j + 1) * n_tile)
            if k is None:
                rhs = g_buf[pl.ds(2 * zz, 2), :, :, cols].reshape(-1, n_tile)
            else:
                rhs = g_buf[pl.ds(2 * zz, 2), k, :, cols].reshape(-1, n_tile)
            term = jnp.dot(lhs, rhs, preferred_element_type=jnp.float32) * scale
            if first:
                gw_ref[:, cols] = term
            else:
                gw_ref[:, cols] += term

    def await_acts(zz, first):
        if split:
            for c in range(2):
                for q in peers:
                    spread_landing(2 * zz + c, q).wait_recv()
        elif first:
            for q in peers:
                spread_all_landing(q).wait_recv()

    def chip_terms(zz, first=False):
        other = 2 * zz + 1 - core
        for k in range(CHUNKS):
            across(other, k).wait_recv()
        await_acts(zz, first)
        accumulate(zz, first)

    def terms_at(d):
        if d == 0:
            chip_terms(z, True)
            return

        @pl.when(z >= d)
        def _():
            chip_terms(z - d)

        @pl.when(z + d < n_line)
        def _():
            chip_terms(z + d)

    def sum_parts():
        for q in peers:
            part_landing(q).wait_recv()
        total = part[tp].astype(jnp.float32)
        for q in peers:
            total = total + landed[q].astype(jnp.float32)
        gin_ref[...] = total.astype(jnp.bfloat16)

    def from_below(d, k):
        s = me - 2 * d
        up(s, k).wait_recv()

        @pl.when(has_up)
        def _():
            up(s, k).start()

        across(s, k).start()

    def from_above(d, k):
        s = me + 2 * d
        down(s, k).wait_recv()

        @pl.when(has_down)
        def _():
            down(s, k).start()

        across(s, k).start()

    for d in range(1, n_line - 1):
        for k in range(CHUNKS):

            @pl.when(z >= d)
            def _():
                from_below(d, k)

            @pl.when(z + d < n_line)
            def _():
                from_above(d, k)

        terms_at(d - 1)

    d = n_line - 1
    terms_at(d - 1)

    def last_terms(zz, arrive):
        other = 2 * zz + 1 - core
        await_acts(zz, False)
        for k in range(CHUNKS):
            arrive(d, k)
            if k == CHUNKS - 1:
                sum_parts()
            if k > 0:
                across(other, k - 1).wait_recv()
                accumulate(zz, False, k - 1)
        across(other, CHUNKS - 1).wait_recv()
        accumulate(zz, False, CHUNKS - 1)

    @pl.when(z == d)
    def _():
        last_terms(0, from_below)

    @pl.when(z == 0)
    def _():
        last_terms(d, from_above)

    @pl.when((z > 0) & (z < d))
    def _():
        sum_parts()

    for r in range(1, n_ctx):
        act_copy(lax.rem(me + r, n_ctx)).wait_send()
    for q in peers:
        part_copy(q).wait_send()
        if split:
            for s in range(n_ctx):
                spread_copy(s, q).wait_send()
        else:
            spread_all(q).wait_send()
    for zz in range(n_line):
        for k in range(CHUNKS):
            s = 2 * zz + core
            across(s, k).wait_send()

            @pl.when(has_up & (zz <= z))
            def _():
                up(s, k).wait_send()

            @pl.when(has_down & (zz >= z))
            def _():
                down(s, k).wait_send()


def line_body(act_codes, scale_exps, weight, grad_out):
    n_ctx, n_tp = lax.axis_size("ctx"), lax.axis_size("tp")
    n_line = n_ctx // 2
    rows, width = act_codes.shape
    toks, cols = grad_out.shape
    feats = width // n_ctx
    d_tile = min(512, width)
    dma = pltpu.SemaphoreType.DMA
    lanes = -(-cols // 128) * 128
    outs = -(-rows // 16) * 16 * width * 2 + feats * lanes * 4
    vmem = pl.BlockSpec(memory_space=pltpu.VMEM)
    hbm = pl.BlockSpec(memory_space=pltpu.HBM)
    bf16 = jnp.bfloat16
    return pl.pallas_call(
        functools.partial(line_kernel, n_ctx, n_tp, toks * n_ctx),
        out_shape=(
            pltpu.VMEM((rows, width), bf16),
            pltpu.VMEM((feats, cols), jnp.float32),
        ),
        in_specs=[hbm, hbm, hbm, hbm],
        out_specs=(vmem, vmem),
        scratch_shapes=[
            pltpu.VMEM((rows, width), bf16),
            pltpu.VMEM(scale_exps.shape[::-1], scale_exps.dtype),
            pltpu.VMEM((width // d_tile, d_tile, cols), bf16),
            pltpu.VMEM((n_ctx, CHUNKS, toks // CHUNKS, cols), bf16),
            pltpu.VMEM((n_ctx, rows, feats), bf16),
            pltpu.VMEM((n_ctx, n_tp, rows, feats), bf16),
            pltpu.VMEM((n_tp, rows, width), bf16),
            pltpu.VMEM((n_tp, rows, width), bf16),
            dma((2,)),
            dma((width // d_tile,)),
            dma((CHUNKS,)),
            dma((n_ctx,)),
            dma((n_ctx,)),
            dma((n_ctx if n_ctx * n_tp <= 64 else 1, n_tp)),
            dma((n_ctx if n_ctx * n_tp <= 64 else 1, n_tp)),
            dma((n_line, CHUNKS)),
            dma((n_line, CHUNKS)),
            dma((n_line, CHUNKS)),
            dma((n_ctx, CHUNKS)),
            dma((n_tp,)),
            dma((n_tp,)),
        ],
        compiler_params=pltpu.CompilerParams(
            collective_id=0, has_side_effects=True, vmem_limit_bytes=67_043_328 - outs - 8192
        ),
    )(act_codes, scale_exps.T, weight, grad_out)


RAW = 1
WIDE = 256


def wide_blocks(cols):
    return cols // WIDE * 3 // 6


def blocks_of(cols):
    full = wide_blocks(cols)
    slim = WIDE // 2
    return [(b * WIDE, WIDE) for b in range(full)] + [
        (start, slim) for start in range(full * WIDE, cols, slim)
    ]


def square_kernel(
    n_ctx, n_tp, tokens,
    codes_hbm, exps_hbm, weight_ref, grads_ref,
    gin_ref, gw_ref,
    codes_ref, exps_ref, w_buf, g_own, g_wide, g_slim, a_send, a_buf, p_buf, a_t, p_t,
    part, recv1, total1, recv2, sums_out, sums_in, slim_out, slim_in,
    in_sem, w_sem, s_sem, line_sem, near_sem, rest_sem, g_rsem, mate_sem,
    one_sem, two_sem, sum_sem,
):
    me = lax.axis_index("ctx")
    tp = lax.axis_index("tp")
    core = lax.rem(me, 2)
    z = lax.div(me, 2)
    mate = me + 1 - 2 * core
    n_line = n_ctx // 2
    side = lax.div(z, 2)
    z_end, z_mid = (n_line - 1) * side, 1 + side
    z_far_mid, z_far_end = 2 - side, (n_line - 1) * (1 - side)
    y, x = lax.div(tp, 2), lax.rem(tp, 2)
    by_x, by_y = 2 * y + 1 - x, 2 * (1 - y) + x
    near = by_x + core * (by_y - by_x)
    next_ = by_y + core * (by_x - by_y)
    diag = n_tp - 1 - tp
    rows, width = codes_ref.shape
    toks = g_own.shape[0]
    block = width // exps_ref.shape[0]
    feats = width // n_ctx
    d_tile = w_buf.shape[1]
    n_d = w_buf.shape[0]
    chip = 2 * toks
    unit = rows * feats
    scale = lax.rsqrt(jnp.float32(tokens))
    blocks = blocks_of(g_own.shape[1])
    n_b = len(blocks)
    full = g_wide.shape[0]

    def g_at(b):
        return g_wide.at[b] if b < full else g_slim.at[b - full]

    def g_piece(s, b):
        return g_at(b).at[pl.ds(s * toks, toks)]

    def load_w(i):
        return pltpu.make_async_copy(
            weight_ref.at[pl.ds(i * d_tile, d_tile)], w_buf.at[i], w_sem.at[i % 2]
        )

    def load_g(b):
        start, size = blocks[b]
        return pltpu.make_async_copy(
            grads_ref.at[:, pl.ds(start, size)], g_piece(me, b), in_sem.at[3]
        )

    load_codes = pltpu.make_async_copy(codes_hbm, codes_ref, in_sem.at[0])
    load_exps = pltpu.make_async_copy(exps_hbm, exps_ref, in_sem.at[1])
    load_own = pltpu.make_async_copy(grads_ref, g_own, in_sem.at[2])
    load_codes.start()
    load_exps.start()
    for b in range(n_b):
        load_g(b).start()

    barrier = pltpu.get_barrier_semaphore()
    for r in range(1, n_ctx):
        pl.semaphore_signal(
            barrier, inc=1, device_id=(lax.rem(me + r, n_ctx), tp), device_id_type=MESH
        )
    for r in range(1, n_tp):
        pl.semaphore_signal(
            barrier, inc=1, device_id=(me, lax.rem(tp + r, n_tp)), device_id_type=MESH
        )
    load_exps.wait()
    load_codes.wait()
    load_w(0).start()
    load_w(1).start()
    powers = jnp.exp2(exps_ref[...].astype(jnp.float32)).T
    for b in range(width // block):
        owner, place = divmod(b * block, feats)
        value = codes_ref[:, b * block : (b + 1) * block].astype(jnp.float32)
        value = value * powers[:, b : b + 1]
        a_send[owner, :, place : place + block] = value.astype(jnp.bfloat16)
    a_buf[me, tp] = a_send[me]
    p_buf[me, tp] = a_send[2 * (z_mid + z_end - z) + core]
    pltpu.make_async_copy(grads_ref, g_own, in_sem.at[3]).wait()
    load_own.start()
    pl.semaphore_wait(barrier, n_ctx + n_tp - 2)

    def program(is_mid):
        sent = {}

        def remote(src, dst, ssem, rsem, to):
            return pltpu.make_async_remote_copy(
                src_ref=src, dst_ref=dst, send_sem=ssem, recv_sem=rsem,
                device_id=to, device_id_type=MESH,
            )

        def send(kind, src, dst, rsem, to):
            remote(src, dst, s_sem.at[kind], rsem, to).start()
            sent[kind] = sent.get(kind, 0) + math.prod(src.shape) // unit

        def landed(dst, rsem):
            remote(dst, dst, s_sem.at[0], rsem, (me, tp)).wait_recv()

        def all_sent():
            for kind, n in sent.items():
                if n % 24 == 0:
                    ref = w_buf.at[pl.ds(0, n // 24)]
                elif n % 2 == 0 and n // 2 <= n_d:
                    ref = recv1.at[pl.ds(0, n // 2)]
                elif n <= n_d:
                    ref = recv2.at[pl.ds(0, n)]
                elif n % 3 == 0 and n // 3 <= n_d:
                    ref = part.at[pl.ds(0, n // 3), pl.ds(0, 3)]
                else:
                    ref = a_buf.at[pl.ds(0, n // n_tp)]
                assert math.prod(ref.shape) == n * unit
                remote(ref, ref, s_sem.at[kind], near_sem.at[0, 0], (me, tp)).wait_send()

        def both(zz):
            return (2 * zz, 2 * zz + 1)

        acts, ends = (a_buf, 0), (p_buf, 1)

        def act_send(d, to, kind):
            buf, k = kind
            send(0, a_send.at[d], buf.at[me, tp], line_sem.at[k, me], (to, tp))

        def spread(kind, s):
            buf, k = kind
            send(1, buf.at[s, tp], buf.at[s, tp], near_sem.at[k, s], (me, near))
            send(2, buf.at[s, tp], buf.at[s, tp], rest_sem.at[k, lax.div(s, 2)], (me, next_))

        def pass_end(s):
            send(3, p_buf.at[s, tp], a_buf.at[s, tp], line_sem.at[0, s], (2 * z_end + core, tp))

        def arrive(kind, s):
            buf, k = kind
            landed(buf.at[s, tp], line_sem.at[k, s])
            spread(kind, s)
            if k == 1 and is_mid:
                pass_end(s)

        def relay(kind, s):
            buf, k = kind
            landed(buf.at[s, near], near_sem.at[k, s])
            send(4, buf.at[s, near], buf.at[s, near], rest_sem.at[k, lax.div(s, 2)], (me, next_))

        def gathered(kind, zz):
            buf, k = kind
            landed(buf.at[2 * zz], rest_sem.at[k, zz])

        def pass_back(s, q):
            send(
                3, p_buf.at[s, q], a_buf.at[s, q], rest_sem.at[0, lax.div(s, 2)],
                (2 * z_mid + core, tp),
            )

        def turned(kind, zz):
            buf, k = kind
            value = buf[pl.ds(2 * zz, 2)].reshape(chip, feats).T
            if k == 0:
                a_t[:, pl.ds(pl.multiple_of(zz * chip, chip), chip)] = value
            else:
                p_t[:, pl.ds(pl.multiple_of((zz - 1 + side) * chip, chip), chip)] = value

        def turn(kind, zz):
            gathered(kind, zz)
            turned(kind, zz)

        def turn_whole(zz):
            landed(a_buf.at[pl.ds(2 * zz, 2)], rest_sem.at[0, zz])
            turned(acts, zz)

        def g_send(kind, s, b, rsem, to):
            send(kind, g_piece(s, b), g_piece(s, b), rsem, (to, tp))

        inward = 2 * (z_far_mid if is_mid else z_mid) + core
        outward = 2 * z_end + core
        FROM_SIDE, FROM_MID, FROM_END = 0, 1, 2

        def g_mine(b):
            g_send(5, me, b, g_rsem.at[FROM_MID if is_mid else FROM_SIDE, b], inward)
            if is_mid and b < RAW:
                g_send(6, me, b, g_rsem.at[FROM_SIDE, b], outward)
            g_send(7, me, b, mate_sem.at[b], mate)

        def g_take(zz, way, b):
            s = 2 * zz + core
            landed(g_piece(s, b), g_rsem.at[way, b])
            if is_mid and way == FROM_SIDE:
                g_send(5, s, b, g_rsem.at[FROM_END, b], inward)
            elif is_mid and b < RAW:
                g_send(6, s, b, g_rsem.at[way, b], outward)
            g_send(7, s, b, mate_sem.at[b], mate)

        def g_mates(n, b):
            landed(g_at(b).at[pl.ds(0, n * toks)], mate_sem.at[b])

        def piece(i):
            if i == 0:
                load_own.wait()
            load_w(i).wait()
            if i + 2 < n_d:
                load_w(i + 2).start()
            value = lax.dot_general(
                g_own[...], w_buf[i], (((1,), (1,)), ((), ())), preferred_element_type=jnp.float32
            ).astype(jnp.bfloat16)
            value = value.reshape(n_tp, rows, d_tile)
            for q in range(n_tp):
                dy, dx = lax.rem(y + q // 2, 2), lax.rem(x + q % 2, 2)
                slot = 2 * dx + dy + core * (dy - dx)
                part[i, slot] = value[q]

        def part_one(i):
            send(8, part.at[i, pl.ds(2, 2)], recv1.at[i], one_sem.at[i], (me, near))

        def part_two(i):
            landed(recv1.at[i], one_sem.at[i])
            total = part[i, 1].astype(jnp.float32) + recv1[i, 1].astype(jnp.float32)
            total1[i] = total.astype(jnp.bfloat16)
            send(9, total1.at[i], recv2.at[i], two_sem.at[i], (me, next_))

        def part_sum(i):
            landed(recv2.at[i], two_sem.at[i])
            total = part[i, 0].astype(jnp.float32) + recv1[i, 0].astype(jnp.float32)
            total = total + recv2[i].astype(jnp.float32)
            gin_ref[:, i * d_tile : (i + 1) * d_tile] = total.astype(jnp.bfloat16)

        def dot(lhs, rhs):
            return jnp.dot(lhs, rhs, preferred_element_type=jnp.float32)

        halves = [slice(h * (feats // 2), (h + 1) * (feats // 2)) for h in range(2)]

        def cols(b):
            start, size = blocks[b]
            return slice(start, start + size)

        def whole_block(b):
            for half in halves:
                gw_ref[half, cols(b)] = dot(a_t[half], g_at(b)[...]) * scale

        def whole_pair(b):
            start, size = blocks[b]
            for half in halves:
                rhs = jnp.concatenate([g_at(b)[...], g_at(b + 1)[...]], axis=1)
                gw_ref[half, start : start + 2 * size] = dot(a_t[half], rhs) * scale

        def tokens_of(near_side):
            first = (side if near_side else 1 - side) * 2 * chip
            return pl.ds(pl.multiple_of(first, 2 * chip), 2 * chip)

        def rhs_of(b, toks_at):
            if b < full:
                return g_at(b)[toks_at]
            return jnp.concatenate([g_at(b)[toks_at], g_at(b + 1)[toks_at]], axis=1)

        def early_block(b):
            start, toks_at = blocks[b][0], tokens_of(True)
            for half in halves:
                gw_ref[half, start : start + WIDE] = dot(a_t[half, toks_at], rhs_of(b, toks_at))

        def late_block(b):
            start, toks_at = blocks[b][0], tokens_of(False)
            for half in halves:
                term = dot(a_t[half, toks_at], rhs_of(b, toks_at))
                gw_ref[half, start : start + WIDE] = (gw_ref[half, start : start + WIDE] + term) * scale

        def out_at(b):
            return sums_out.at[b - RAW] if b < full else slim_out.at[b - full]

        def in_at(b):
            return sums_in.at[b - RAW] if b < full else slim_in.at[b - full]

        def sum_block(b):
            first = pl.multiple_of((1 - side) * chip, chip)
            for half in halves:
                rhs = g_at(b)[pl.ds(first, (n_line - 1) * chip)]
                out_at(b)[half] = dot(p_t[half], rhs).astype(jnp.bfloat16)
                send(10, out_at(b).at[half], in_at(b).at[half], sum_sem.at[b - RAW], (outward, tp))

        def own_block(b):
            here = pl.ds(pl.multiple_of(z_end * chip, chip), chip)
            for half in halves:
                gw_ref[half, cols(b)] = dot(a_t[half, here], g_at(b)[here])

        def add_block(b):
            landed(in_at(b), sum_sem.at[b - RAW])
            gw_ref[:, cols(b)] = (gw_ref[:, cols(b)] + in_at(b)[...].astype(jnp.float32)) * scale

        if is_mid:
            for c in range(2):
                act_send(2 * z_far_end + c, 2 * z_far_mid + c, ends)
            g_mine(1)
            g_mine(0)
            g_mine(3)
            pass_end(me)
            act_send(2 * z_end + 1 - core, mate, ends)
            spread(ends, me)
            spread(acts, me)
            act_send(mate, mate, acts)
            piece(0)
            piece(1)
            arrive(ends, mate)
            arrive(acts, mate)
            piece(2)
            piece(3)
            piece(4)
            arrive(ends, 2 * z_far_mid + core)
            piece(5)
            piece(6)
            relay(ends, me)
            arrive(ends, 2 * z_far_mid + 1 - core)
            g_take(z_end, FROM_SIDE, 1)
            piece(7)
            relay(acts, me)
            relay(ends, mate)
            arrive(ends, 2 * z_far_end + core)
            relay(acts, mate)
            relay(ends, 2 * z_far_mid + core)
            g_take(z_far_mid, FROM_MID, 1)
            arrive(ends, 2 * z_far_end + 1 - core)
            relay(ends, 2 * z_far_mid + 1 - core)
            relay(ends, 2 * z_far_end + core)
            g_take(z_far_mid, FROM_MID, 0)
            g_take(z_far_mid, FROM_MID, 3)
            turn(ends, z_mid)
            g_take(z_end, FROM_SIDE, 0)
            part_one(0)
            relay(ends, 2 * z_far_end + 1 - core)
            turn(acts, z_mid)
            g_take(z_far_end, FROM_END, 1)
            g_take(z_end, FROM_SIDE, 2)
            g_mine(2)
            g_mates(n_line, 1)
            part_one(1)
            turn(ends, z_far_mid)
            g_take(z_far_end, FROM_END, 0)
            part_two(0)
            turn(ends, z_far_end)
            g_mates(n_line, 0)
            g_take(z_end, FROM_SIDE, 3)
            for c in range(2):
                act_send(2 * z_far_mid + c, 2 * z_far_mid + c, acts)
            sum_block(1)
            g_take(z_far_end, FROM_END, 2)
            part_two(1)
            g_take(z_far_mid, FROM_MID, 2)
            g_take(z_end, FROM_SIDE, 4)
            g_mine(4)
            g_mine(5)
            g_take(z_end, FROM_SIDE, 5)
            g_mine(6)
            part_one(2)
            part_one(3)
            g_mates(n_line, 2)
            sum_block(2)
            g_take(z_far_end, FROM_END, 3)
            part_one(4)
            part_one(5)
            g_mates(n_line, 3)
            sum_block(3)
            arrive(acts, 2 * z_far_mid + core)
            arrive(acts, 2 * z_far_end + core)
            part_two(2)
            part_two(3)
            arrive(acts, 2 * z_far_mid + 1 - core)
            arrive(acts, 2 * z_far_end + 1 - core)
            g_take(z_far_end, FROM_END, 4)
            g_take(z_end, FROM_SIDE, 6)
            g_mine(7)
            g_take(z_end, FROM_SIDE, 7)
            g_mine(8)
            g_take(z_end, FROM_SIDE, 8)
            part_two(4)
            part_one(6)
            part_one(7)
            g_take(z_far_mid, FROM_MID, 4)
            g_mates(n_line, 4)
            sum_block(4)
            g_take(z_far_mid, FROM_MID, 5)
            g_take(z_far_end, FROM_END, 5)
            part_two(5)
            g_mates(n_line, 5)
            sum_block(5)
            relay(acts, 2 * z_far_mid + core)
            g_take(z_far_mid, FROM_MID, 6)
            g_take(z_far_end, FROM_END, 6)
            relay(acts, 2 * z_far_end + core)
            turn_whole(z_end)
            g_mates(n_line, 6)
            sum_block(6)
            relay(acts, 2 * z_far_mid + 1 - core)
            g_take(z_far_mid, FROM_MID, 7)
            g_take(z_far_end, FROM_END, 7)
            relay(acts, 2 * z_far_end + 1 - core)
            early_block(0)
            g_mates(n_line, 7)
            sum_block(7)
            g_take(z_far_mid, FROM_MID, 8)
            g_take(z_far_end, FROM_END, 8)
            early_block(1)
            g_mates(n_line, 8)
            sum_block(8)
            early_block(2)
            early_block(3)
            early_block(5)
            part_two(6)
            turn(acts, z_far_mid)
            turn(acts, z_far_end)
            late_block(0)
            late_block(1)
            part_two(7)
            late_block(2)
            late_block(3)
            late_block(5)
            whole_pair(7)
            part_sum(0)
            part_sum(1)
            part_sum(2)
            part_sum(3)
            part_sum(4)
            part_sum(5)
            part_sum(6)
            part_sum(7)
        else:
            act_send(2 * z_mid + 1 - core, mate, ends)
            spread(ends, me)
            act_send(mate, mate, acts)
            g_mine(1)
            for c in range(2):
                act_send(2 * z_far_end + c, 2 * z_far_mid + c, ends)
            pass_back(me, tp)
            g_mine(0)
            g_mine(2)
            spread(acts, me)
            piece(0)
            piece(1)
            arrive(ends, mate)
            arrive(acts, mate)
            part_one(0)
            piece(2)
            piece(3)
            piece(4)
            piece(5)
            piece(6)
            relay(ends, me)
            g_take(z_mid, FROM_SIDE, 0)
            piece(7)
            part_one(1)
            relay(acts, me)
            part_one(2)
            arrive(acts, 2 * z_mid + core)
            relay(ends, mate)
            arrive(acts, 2 * z_mid + 1 - core)
            part_one(3)
            relay(acts, mate)
            arrive(acts, 2 * z_far_mid + core)
            arrive(acts, 2 * z_far_mid + 1 - core)
            part_one(4)
            part_one(5)
            part_two(0)
            arrive(acts, 2 * z_far_end + core)
            part_one(6)
            gathered(ends, z_end)
            pass_back(me, diag)
            g_mine(7)
            g_mine(3)
            g_mine(5)
            g_mine(8)
            g_mine(4)
            pass_back(me, near)
            for c in range(2):
                act_send(2 * z_far_mid + c, 2 * z_far_mid + c, acts)
            g_mine(6)
            pass_back(mate, near)
            pass_back(me, next_)
            pass_back(mate, diag)
            pass_back(mate, next_)
            pass_back(mate, tp)
            arrive(acts, 2 * z_far_end + 1 - core)
            part_two(1)
            part_one(7)
            turn(acts, z_end)
            g_mates(1, 1)
            own_block(1)
            g_mates(1, 2)
            own_block(2)
            g_mates(1, 3)
            own_block(3)
            g_take(z_far_mid, FROM_MID, 0)
            g_mates(1, 4)
            own_block(4)
            g_mates(1, 5)
            own_block(5)
            relay(acts, 2 * z_mid + core)
            g_mates(1, 6)
            own_block(6)
            g_mates(1, 7)
            own_block(7)
            g_mates(1, 8)
            own_block(8)
            part_two(2)
            relay(acts, 2 * z_mid + 1 - core)
            part_sum(0)
            part_two(3)
            relay(acts, 2 * z_far_mid + core)
            g_take(z_far_end, FROM_END, 0)
            relay(acts, 2 * z_far_mid + 1 - core)
            part_sum(1)
            g_mates(n_line, 0)
            part_sum(2)
            part_two(4)
            turn(acts, z_mid)
            add_block(1)
            part_sum(3)
            part_two(5)
            relay(acts, 2 * z_far_end + core)
            turn(acts, z_far_mid)
            part_sum(4)
            part_two(6)
            add_block(2)
            relay(acts, 2 * z_far_end + 1 - core)
            part_sum(5)
            add_block(3)
            part_two(7)
            part_sum(6)
            turn(acts, z_far_end)
            whole_block(0)
            add_block(4)
            part_sum(7)
            add_block(5)
            add_block(6)
            add_block(7)
            add_block(8)
        all_sent()

    is_mid = z == z_mid

    @pl.when(is_mid)
    def _():
        program(True)

    @pl.when(jnp.logical_not(is_mid))
    def _():
        program(False)


def square_body(act_codes, scale_exps, weight, grad_out):
    n_ctx, n_tp = lax.axis_size("ctx"), lax.axis_size("tp")
    rows, width = act_codes.shape
    toks, cols = grad_out.shape
    feats = width // n_ctx
    d_tile = width // 8
    n_d = width // d_tile
    all_toks = toks * n_ctx
    n_b = len(blocks_of(cols))
    full = wide_blocks(cols)
    dma = pltpu.SemaphoreType.DMA
    vmem = pl.BlockSpec(memory_space=pltpu.VMEM)
    hbm = pl.BlockSpec(memory_space=pltpu.HBM)
    bf16 = jnp.bfloat16
    outs = rows * width * 2 + feats * cols * 4
    gin, gw = pl.pallas_call(
        functools.partial(square_kernel, n_ctx, n_tp, all_toks),
        out_shape=(
            pltpu.VMEM((rows, width), bf16),
            pltpu.VMEM((feats, cols), jnp.float32),
        ),
        in_specs=[hbm, hbm, hbm, hbm],
        out_specs=(vmem, vmem),
        scratch_shapes=[
            pltpu.VMEM((rows, width), bf16),
            pltpu.VMEM(scale_exps.shape[::-1], scale_exps.dtype),
            pltpu.VMEM((n_d, d_tile, cols), bf16),
            pltpu.VMEM((toks, cols), bf16),
            pltpu.VMEM((full, all_toks, WIDE), bf16),
            pltpu.VMEM((n_b - full, all_toks, WIDE // 2), bf16),
            pltpu.VMEM((n_ctx, rows, feats), bf16),
            pltpu.VMEM((n_ctx, n_tp, rows, feats), bf16),
            pltpu.VMEM((n_ctx, n_tp, rows, feats), bf16),
            pltpu.VMEM((feats, all_toks), bf16),
            pltpu.VMEM((feats, all_toks - 2 * toks), bf16),
            pltpu.VMEM((n_d, n_tp, rows, d_tile), bf16),
            pltpu.VMEM((n_d, 2, rows, d_tile), bf16),
            pltpu.VMEM((n_d, rows, d_tile), bf16),
            pltpu.VMEM((n_d, rows, d_tile), bf16),
            pltpu.VMEM((max(full - RAW, 1), feats, WIDE), bf16),
            pltpu.VMEM((max(full - RAW, 1), feats, WIDE), bf16),
            pltpu.VMEM((n_b - full, feats, WIDE // 2), bf16),
            pltpu.VMEM((n_b - full, feats, WIDE // 2), bf16),
            dma((4,)),
            dma((2,)),
            dma((11,)),
            dma((2, n_ctx)),
            dma((2, n_ctx)),
            dma((2, n_ctx // 2)),
            dma((3, n_b)),
            dma((n_b,)),
            dma((n_d,)),
            dma((n_d,)),
            dma((n_b - RAW,)),
        ],
        compiler_params=pltpu.CompilerParams(
            collective_id=0, has_side_effects=True, vmem_limit_bytes=67_043_328 - outs - 8192
        ),
    )(act_codes, scale_exps.T, weight, grad_out)
    return pl.pallas_call(
        store_kernel,
        out_shape=(
            jax.ShapeDtypeStruct(gin.shape, gin.dtype), jax.ShapeDtypeStruct(gw.shape, gw.dtype)
        ),
        in_specs=[vmem, vmem],
        out_specs=(hbm, hbm),
        scratch_shapes=[dma((2,))],
        compiler_params=pltpu.CompilerParams(vmem_limit_bytes=1 << 20),
    )(gin, gw)


def store_kernel(gin_ref, gw_ref, gin_out, gw_out, sem):
    copies = [
        pltpu.make_async_copy(gw_ref, gw_out, sem.at[0]),
        pltpu.make_async_copy(gin_ref, gin_out, sem.at[1]),
    ]
    for copy in copies:
        copy.start()
    for copy in copies:
        copy.wait()


def body(act_codes, scale_exps, weight, grad_out):
    line, square = lax.axis_size("ctx") // 2, lax.axis_size("tp")
    if line == 4 and square == 4 and grad_out.shape[1] % WIDE == 0:
        return square_body(act_codes, scale_exps, weight, grad_out)
    return line_body(act_codes, scale_exps, weight, grad_out)


def solution(mesh):
    placed = (P(("ctx", "tp"), None), P(("ctx", "tp"), None), P(None, "tp"), P("ctx", "tp"))
    return jax.shard_map(
        body,
        mesh=mesh,
        in_specs=placed,
        out_specs=(P(("ctx", "tp"), None), P("ctx", "tp")),
        check_vma=False,
    )
```

```python
import functools
import math

import jax
import jax.numpy as jnp
from jax import lax
from jax.experimental import pallas as pl
from jax.experimental.pallas import tpu as pltpu
from jax.sharding import PartitionSpec as P

MESH = pl.DeviceIdType.MESH
CHUNKS = 4


def line_kernel(
    n_ctx, n_tp, tokens,
    codes_hbm, exps_hbm, weight_ref, grads_ref,
    gin_ref, gw_ref,
    codes_ref, exps_ref, w_buf, g_buf, a_send, a_buf, part, landed,
    in_sem, w_sem, g_sem,
    a_ssem, a_rsem, b_ssem, b_rsem, up_ssem, down_ssem, mate_ssem, g_rsem, p_ssem, p_rsem,
):
    n_line = n_ctx // 2
    me = lax.axis_index("ctx")
    tp = lax.axis_index("tp")
    core = lax.rem(me, 2)
    z = lax.div(me, 2)
    mate = me + 1 - 2 * core
    rows, width = codes_ref.shape
    block = width // exps_ref.shape[0]
    feats = width // n_ctx
    d_tile = w_buf.shape[1]
    n_d = w_buf.shape[0]
    scale = lax.rsqrt(jnp.float32(tokens))
    split = n_ctx * n_tp <= 64

    def load_w(i):
        return pltpu.make_async_copy(
            weight_ref.at[pl.ds(i * d_tile, d_tile)], w_buf.at[i], w_sem.at[i]
        )

    def load_g(k):
        size = g_buf.shape[2]
        return pltpu.make_async_copy(
            grads_ref.at[pl.ds(k * size, size)], g_buf.at[me, k], g_sem.at[k]
        )

    load_codes = pltpu.make_async_copy(codes_hbm, codes_ref, in_sem.at[0])
    load_exps = pltpu.make_async_copy(exps_hbm, exps_ref, in_sem.at[1])
    load_g(0).start()
    load_codes.start()
    load_exps.start()
    for k in range(1, CHUNKS):
        load_g(k).start()
    for i in range(n_d):
        load_w(i).start()

    barrier = pltpu.get_barrier_semaphore()
    for r in range(1, n_ctx):
        pl.semaphore_signal(
            barrier, inc=1, device_id=(lax.rem(me + r, n_ctx), tp), device_id_type=MESH
        )
    for r in range(1, n_tp):
        pl.semaphore_signal(
            barrier, inc=1, device_id=(me, lax.rem(tp + r, n_tp)), device_id_type=MESH
        )

    pl.semaphore_wait(barrier, n_ctx + n_tp - 2)

    def remote(src, dst, ssem, rsem, to):
        return pltpu.make_async_remote_copy(
            src_ref=src, dst_ref=dst, send_sem=ssem, recv_sem=rsem,
            device_id=to, device_id_type=MESH,
        )

    def act_copy(to):
        return remote(
            a_send.at[to], a_buf.at[me, tp], a_ssem.at[to], a_rsem.at[me], (to, tp)
        )

    def act_landing(source):
        return remote(
            a_send.at[source], a_buf.at[source, tp], a_ssem.at[source], a_rsem.at[source],
            (source, tp),
        )

    def spread_copy(s, q, src=None):
        return remote(
            a_buf.at[s, tp] if src is None else src,
            a_buf.at[s, tp], b_ssem.at[s, q], b_rsem.at[s, tp], (me, q),
        )

    def spread_landing(s, q):
        return remote(
            a_buf.at[s, q], a_buf.at[s, q], b_ssem.at[s, q], b_rsem.at[s, q], (me, q)
        )

    def spread_all(q):
        return remote(
            a_buf.at[:, tp], a_buf.at[:, tp], b_ssem.at[0, q], b_rsem.at[0, tp], (me, q)
        )

    def spread_all_landing(q):
        return remote(
            a_buf.at[:, q], a_buf.at[:, q], b_ssem.at[0, q], b_rsem.at[0, q], (me, q)
        )

    def pass_on(s, k, ssem, to):
        return remote(
            g_buf.at[s, k], g_buf.at[s, k], ssem.at[lax.div(s, 2), k], g_rsem.at[s, k], (to, tp)
        )

    def up(s, k):
        return pass_on(s, k, up_ssem, me + 2)

    def down(s, k):
        return pass_on(s, k, down_ssem, me - 2)

    def across(s, k):
        return pass_on(s, k, mate_ssem, mate)

    has_up = z < n_line - 1
    has_down = z > 0

    def send_own(k):
        load_g(k).wait()

        @pl.when(has_up)
        def _():
            up(me, k).start()

        @pl.when(has_down)
        def _():
            down(me, k).start()

        across(me, k).start()

    send_own(0)
    load_codes.wait()
    load_exps.wait()
    powers = jnp.exp2(exps_ref[...].astype(jnp.float32)).T
    for b in range(width // block):
        owner, place = divmod(b * block, feats)
        value = codes_ref[:, b * block : (b + 1) * block].astype(jnp.float32)
        value = value * powers[:, b : b + 1]
        a_send[owner, :, place : place + block] = value.astype(jnp.bfloat16)
    a_buf[me, tp] = a_send[me]
    for r in range(1, n_ctx):
        act_copy(lax.rem(me + r, n_ctx)).start()
    for k in range(1, CHUNKS):
        send_own(k)

    peers = [lax.rem(tp + r, n_tp) for r in range(1, n_tp)]
    if split:
        for q in peers:
            spread_copy(me, q, a_send.at[me]).start()

    grads = g_buf.at[me]

    def part_piece(i):
        load_w(i).wait()
        rows_all = grads[...].reshape(-1, g_buf.shape[3])
        piece = lax.dot_general(
            rows_all, w_buf[i], (((1,), (1,)), ((), ())), preferred_element_type=jnp.float32
        ).astype(jnp.bfloat16)
        part[:, :, i * d_tile : (i + 1) * d_tile] = piece.reshape(n_tp, rows, d_tile)

    per = -(-n_d // n_ctx)
    done = 0
    for r in range(1, n_ctx):
        for i in range(done, min(done + per, n_d)):
            part_piece(i)
        done = min(done + per, n_d)
        s = lax.rem(me - r + n_ctx, n_ctx)
        act_landing(s).wait_recv()
        if split:
            for q in peers:
                spread_copy(s, q).start()
    for i in range(done, n_d):
        part_piece(i)
    if not split:
        for q in peers:
            spread_all(q).start()

    def part_copy(q):
        return remote(part.at[q], landed.at[tp], p_ssem.at[q], p_rsem.at[tp], (me, q))

    def part_landing(q):
        return remote(part.at[q], landed.at[q], p_ssem.at[q], p_rsem.at[q], (me, q))

    for q in peers:
        part_copy(q).start()

    n_cols = g_buf.shape[3]
    n_tile = 512 if n_cols % 512 == 0 else n_cols

    def accumulate(zz, first, k=None):
        if k is None:
            lhs = a_buf[pl.ds(2 * zz, 2)].reshape(-1, feats).T
        else:
            size = n_tp // CHUNKS
            lhs = a_buf[pl.ds(2 * zz, 2), k * size : (k + 1) * size].reshape(-1, feats).T

        for j in range(n_cols // n_tile):
            cols = slice(j * n_tile, (j + 1) * n_tile)
            if k is None:
                rhs = g_buf[pl.ds(2 * zz, 2), :, :, cols].reshape(-1, n_tile)
            else:
                rhs = g_buf[pl.ds(2 * zz, 2), k, :, cols].reshape(-1, n_tile)
            term = jnp.dot(lhs, rhs, preferred_element_type=jnp.float32) * scale
            if first:
                gw_ref[:, cols] = term
            else:
                gw_ref[:, cols] += term

    def await_acts(zz, first):
        if split:
            for c in range(2):
                for q in peers:
                    spread_landing(2 * zz + c, q).wait_recv()
        elif first:
            for q in peers:
                spread_all_landing(q).wait_recv()

    def chip_terms(zz, first=False):
        other = 2 * zz + 1 - core
        for k in range(CHUNKS):
            across(other, k).wait_recv()
        await_acts(zz, first)
        accumulate(zz, first)

    def terms_at(d):
        if d == 0:
            chip_terms(z, True)
            return

        @pl.when(z >= d)
        def _():
            chip_terms(z - d)

        @pl.when(z + d < n_line)
        def _():
            chip_terms(z + d)

    def sum_parts():
        for q in peers:
            part_landing(q).wait_recv()
        total = part[tp].astype(jnp.float32)
        for q in peers:
            total = total + landed[q].astype(jnp.float32)
        gin_ref[...] = total.astype(jnp.bfloat16)

    def from_below(d, k):
        s = me - 2 * d
        up(s, k).wait_recv()

        @pl.when(has_up)
        def _():
            up(s, k).start()

        across(s, k).start()

    def from_above(d, k):
        s = me + 2 * d
        down(s, k).wait_recv()

        @pl.when(has_down)
        def _():
            down(s, k).start()

        across(s, k).start()

    for d in range(1, n_line - 1):
        for k in range(CHUNKS):

            @pl.when(z >= d)
            def _():
                from_below(d, k)

            @pl.when(z + d < n_line)
            def _():
                from_above(d, k)

        terms_at(d - 1)

    d = n_line - 1
    terms_at(d - 1)

    def last_terms(zz, arrive):
        other = 2 * zz + 1 - core
        await_acts(zz, False)
        for k in range(CHUNKS):
            arrive(d, k)
            if k == CHUNKS - 1:
                sum_parts()
            if k > 0:
                across(other, k - 1).wait_recv()
                accumulate(zz, False, k - 1)
        across(other, CHUNKS - 1).wait_recv()
        accumulate(zz, False, CHUNKS - 1)

    @pl.when(z == d)
    def _():
        last_terms(0, from_below)

    @pl.when(z == 0)
    def _():
        last_terms(d, from_above)

    @pl.when((z > 0) & (z < d))
    def _():
        sum_parts()

    for r in range(1, n_ctx):
        act_copy(lax.rem(me + r, n_ctx)).wait_send()
    for q in peers:
        part_copy(q).wait_send()
        if split:
            for s in range(n_ctx):
                spread_copy(s, q).wait_send()
        else:
            spread_all(q).wait_send()
    for zz in range(n_line):
        for k in range(CHUNKS):
            s = 2 * zz + core
            across(s, k).wait_send()

            @pl.when(has_up & (zz <= z))
            def _():
                up(s, k).wait_send()

            @pl.when(has_down & (zz >= z))
            def _():
                down(s, k).wait_send()


def line_body(act_codes, scale_exps, weight, grad_out):
    n_ctx, n_tp = lax.axis_size("ctx"), lax.axis_size("tp")
    n_line = n_ctx // 2
    rows, width = act_codes.shape
    toks, cols = grad_out.shape
    feats = width // n_ctx
    d_tile = min(512, width)
    dma = pltpu.SemaphoreType.DMA
    lanes = -(-cols // 128) * 128
    outs = -(-rows // 16) * 16 * width * 2 + feats * lanes * 4
    vmem = pl.BlockSpec(memory_space=pltpu.VMEM)
    hbm = pl.BlockSpec(memory_space=pltpu.HBM)
    bf16 = jnp.bfloat16
    return pl.pallas_call(
        functools.partial(line_kernel, n_ctx, n_tp, toks * n_ctx),
        out_shape=(
            pltpu.VMEM((rows, width), bf16),
            pltpu.VMEM((feats, cols), jnp.float32),
        ),
        in_specs=[hbm, hbm, hbm, hbm],
        out_specs=(vmem, vmem),
        scratch_shapes=[
            pltpu.VMEM((rows, width), bf16),
            pltpu.VMEM(scale_exps.shape[::-1], scale_exps.dtype),
            pltpu.VMEM((width // d_tile, d_tile, cols), bf16),
            pltpu.VMEM((n_ctx, CHUNKS, toks // CHUNKS, cols), bf16),
            pltpu.VMEM((n_ctx, rows, feats), bf16),
            pltpu.VMEM((n_ctx, n_tp, rows, feats), bf16),
            pltpu.VMEM((n_tp, rows, width), bf16),
            pltpu.VMEM((n_tp, rows, width), bf16),
            dma((2,)),
            dma((width // d_tile,)),
            dma((CHUNKS,)),
            dma((n_ctx,)),
            dma((n_ctx,)),
            dma((n_ctx if n_ctx * n_tp <= 64 else 1, n_tp)),
            dma((n_ctx if n_ctx * n_tp <= 64 else 1, n_tp)),
            dma((n_line, CHUNKS)),
            dma((n_line, CHUNKS)),
            dma((n_line, CHUNKS)),
            dma((n_ctx, CHUNKS)),
            dma((n_tp,)),
            dma((n_tp,)),
        ],
        compiler_params=pltpu.CompilerParams(
            collective_id=0, has_side_effects=True, vmem_limit_bytes=67_043_328 - outs - 8192
        ),
    )(act_codes, scale_exps.T, weight, grad_out)


RAW = 1
WIDE = 256


def wide_blocks(cols):
    return cols // WIDE * 3 // 6


def blocks_of(cols):
    full = wide_blocks(cols)
    slim = WIDE // 2
    return [(b * WIDE, WIDE) for b in range(full)] + [
        (start, slim) for start in range(full * WIDE, cols, slim)
    ]


def square_kernel(
    n_ctx, n_tp, tokens,
    codes_hbm, exps_hbm, weight_ref, grads_ref,
    gin_ref, gw_ref,
    codes_ref, exps_ref, w_buf, g_own, g_wide, g_slim, a_send, a_buf, p_buf, a_t, p_t,
    part, recv1, total1, recv2, sums_out, sums_in, slim_out, slim_in,
    in_sem, w_sem, s_sem, line_sem, near_sem, rest_sem, g_rsem, mate_sem,
    one_sem, two_sem, sum_sem,
):
    me = lax.axis_index("ctx")
    tp = lax.axis_index("tp")
    core = lax.rem(me, 2)
    z = lax.div(me, 2)
    mate = me + 1 - 2 * core
    n_line = n_ctx // 2
    side = lax.div(z, 2)
    z_end, z_mid = (n_line - 1) * side, 1 + side
    z_far_mid, z_far_end = 2 - side, (n_line - 1) * (1 - side)
    y, x = lax.div(tp, 2), lax.rem(tp, 2)
    by_x, by_y = 2 * y + 1 - x, 2 * (1 - y) + x
    near = by_x + core * (by_y - by_x)
    next_ = by_y + core * (by_x - by_y)
    diag = n_tp - 1 - tp
    rows, width = codes_ref.shape
    toks = g_own.shape[0]
    block = width // exps_ref.shape[0]
    feats = width // n_ctx
    d_tile = w_buf.shape[1]
    n_d = w_buf.shape[0]
    chip = 2 * toks
    unit = rows * feats
    scale = lax.rsqrt(jnp.float32(tokens))
    blocks = blocks_of(g_own.shape[1])
    n_b = len(blocks)
    full = g_wide.shape[0]

    def g_at(b):
        return g_wide.at[b] if b < full else g_slim.at[b - full]

    def g_piece(s, b):
        return g_at(b).at[pl.ds(s * toks, toks)]

    def load_w(i):
        return pltpu.make_async_copy(
            weight_ref.at[pl.ds(i * d_tile, d_tile)], w_buf.at[i], w_sem.at[i % 2]
        )

    def load_g(b):
        start, size = blocks[b]
        return pltpu.make_async_copy(
            grads_ref.at[:, pl.ds(start, size)], g_piece(me, b), in_sem.at[3]
        )

    load_codes = pltpu.make_async_copy(codes_hbm, codes_ref, in_sem.at[0])
    load_exps = pltpu.make_async_copy(exps_hbm, exps_ref, in_sem.at[1])
    load_own = pltpu.make_async_copy(grads_ref, g_own, in_sem.at[2])
    load_codes.start()
    load_exps.start()
    for b in range(n_b):
        load_g(b).start()

    barrier = pltpu.get_barrier_semaphore()
    end_chip = z != z_mid

    def greet(ctx, square):
        pl.semaphore_signal(barrier, inc=1, device_id=(ctx, square), device_id_type=MESH)

    greet(mate, tp)
    greet(me, near)
    greet(me, next_)

    @pl.when(end_chip)
    def _():
        greet(2 * z_mid + core, tp)

    @pl.when(jnp.logical_not(end_chip))
    def _():
        for zz in (z_end, z_far_mid, z_far_end):
            for c in range(2):
                greet(2 * zz + c, tp)

    load_exps.wait()
    load_codes.wait()
    load_w(0).start()
    load_w(1).start()
    powers = jnp.exp2(exps_ref[...].astype(jnp.float32)).T
    for b in range(width // block):
        owner, place = divmod(b * block, feats)
        value = codes_ref[:, b * block : (b + 1) * block].astype(jnp.float32)
        value = value * powers[:, b : b + 1]
        a_send[owner, :, place : place + block] = value.astype(jnp.bfloat16)
    a_buf[me, tp] = a_send[me]
    p_buf[me, tp] = a_send[2 * (z_mid + z_end - z) + core]
    pltpu.make_async_copy(grads_ref, g_own, in_sem.at[3]).wait()
    load_own.start()
    @pl.when(end_chip)
    def _():
        pl.semaphore_wait(barrier, 7)

    @pl.when(jnp.logical_not(end_chip))
    def _():
        pl.semaphore_wait(barrier, 6)

    def program(is_mid):
        sent = {}

        def remote(src, dst, ssem, rsem, to):
            return pltpu.make_async_remote_copy(
                src_ref=src, dst_ref=dst, send_sem=ssem, recv_sem=rsem,
                device_id=to, device_id_type=MESH,
            )

        def send(kind, src, dst, rsem, to):
            remote(src, dst, s_sem.at[kind], rsem, to).start()
            sent[kind] = sent.get(kind, 0) + math.prod(src.shape) // unit

        def landed(dst, rsem):
            remote(dst, dst, s_sem.at[0], rsem, (me, tp)).wait_recv()

        def all_sent():
            for kind, n in sent.items():
                if n % 24 == 0:
                    ref = w_buf.at[pl.ds(0, n // 24)]
                elif n % 2 == 0 and n // 2 <= n_d:
                    ref = recv1.at[pl.ds(0, n // 2)]
                elif n <= n_d:
                    ref = recv2.at[pl.ds(0, n)]
                elif n % 3 == 0 and n // 3 <= n_d:
                    ref = part.at[pl.ds(0, n // 3), pl.ds(0, 3)]
                else:
                    ref = a_buf.at[pl.ds(0, n // n_tp)]
                assert math.prod(ref.shape) == n * unit
                remote(ref, ref, s_sem.at[kind], near_sem.at[0, 0], (me, tp)).wait_send()

        def both(zz):
            return (2 * zz, 2 * zz + 1)

        acts, ends = (a_buf, 0), (p_buf, 1)

        def act_send(d, to, kind):
            buf, k = kind
            send(0, a_send.at[d], buf.at[me, tp], line_sem.at[k, me], (to, tp))

        def spread(kind, s):
            buf, k = kind
            send(1, buf.at[s, tp], buf.at[s, tp], near_sem.at[k, s], (me, near))
            send(2, buf.at[s, tp], buf.at[s, tp], rest_sem.at[k, lax.div(s, 2)], (me, next_))

        def pass_end(s):
            send(3, p_buf.at[s, tp], a_buf.at[s, tp], line_sem.at[0, s], (2 * z_end + core, tp))

        def arrive(kind, s):
            buf, k = kind
            landed(buf.at[s, tp], line_sem.at[k, s])
            spread(kind, s)
            if k == 1 and is_mid:
                pass_end(s)

        def relay(kind, s):
            buf, k = kind
            landed(buf.at[s, near], near_sem.at[k, s])
            send(4, buf.at[s, near], buf.at[s, near], rest_sem.at[k, lax.div(s, 2)], (me, next_))

        def gathered(kind, zz):
            buf, k = kind
            landed(buf.at[2 * zz], rest_sem.at[k, zz])

        def pass_back(s, q):
            send(
                3, p_buf.at[s, q], a_buf.at[s, q], rest_sem.at[0, lax.div(s, 2)],
                (2 * z_mid + core, tp),
            )

        def turned(kind, zz):
            buf, k = kind
            value = buf[pl.ds(2 * zz, 2)].reshape(chip, feats).T
            if k == 0:
                a_t[:, pl.ds(pl.multiple_of(zz * chip, chip), chip)] = value
            else:
                p_t[:, pl.ds(pl.multiple_of((zz - 1 + side) * chip, chip), chip)] = value

        def turn(kind, zz):
            gathered(kind, zz)
            turned(kind, zz)

        def turn_whole(zz):
            landed(a_buf.at[pl.ds(2 * zz, 2)], rest_sem.at[0, zz])
            turned(acts, zz)

        def g_send(kind, s, b, rsem, to):
            send(kind, g_piece(s, b), g_piece(s, b), rsem, (to, tp))

        inward = 2 * (z_far_mid if is_mid else z_mid) + core
        outward = 2 * z_end + core
        FROM_SIDE, FROM_MID, FROM_END = 0, 1, 2

        def g_mine(b):
            g_send(5, me, b, g_rsem.at[FROM_MID if is_mid else FROM_SIDE, b], inward)
            if is_mid and b < RAW:
                g_send(6, me, b, g_rsem.at[FROM_SIDE, b], outward)
            g_send(7, me, b, mate_sem.at[b], mate)

        def g_take(zz, way, b):
            s = 2 * zz + core
            landed(g_piece(s, b), g_rsem.at[way, b])
            if is_mid and way == FROM_SIDE:
                g_send(5, s, b, g_rsem.at[FROM_END, b], inward)
            elif is_mid and b < RAW:
                g_send(6, s, b, g_rsem.at[way, b], outward)
            g_send(7, s, b, mate_sem.at[b], mate)

        def g_mates(n, b):
            landed(g_at(b).at[pl.ds(0, n * toks)], mate_sem.at[b])

        def piece(i):
            if i == 0:
                load_own.wait()
            load_w(i).wait()
            if i + 2 < n_d:
                load_w(i + 2).start()
            value = lax.dot_general(
                g_own[...], w_buf[i], (((1,), (1,)), ((), ())), preferred_element_type=jnp.float32
            ).astype(jnp.bfloat16)
            value = value.reshape(n_tp, rows, d_tile)
            for q in range(n_tp):
                dy, dx = lax.rem(y + q // 2, 2), lax.rem(x + q % 2, 2)
                slot = 2 * dx + dy + core * (dy - dx)
                part[i, slot] = value[q]

        def part_one(i):
            send(8, part.at[i, pl.ds(2, 2)], recv1.at[i], one_sem.at[i], (me, near))

        def part_two(i):
            landed(recv1.at[i], one_sem.at[i])
            total = part[i, 1].astype(jnp.float32) + recv1[i, 1].astype(jnp.float32)
            total1[i] = total.astype(jnp.bfloat16)
            send(9, total1.at[i], recv2.at[i], two_sem.at[i], (me, next_))

        def part_sum(i):
            landed(recv2.at[i], two_sem.at[i])
            total = part[i, 0].astype(jnp.float32) + recv1[i, 0].astype(jnp.float32)
            total = total + recv2[i].astype(jnp.float32)
            gin_ref[:, i * d_tile : (i + 1) * d_tile] = total.astype(jnp.bfloat16)

        def dot(lhs, rhs):
            return jnp.dot(lhs, rhs, preferred_element_type=jnp.float32)

        halves = [slice(h * (feats // 2), (h + 1) * (feats // 2)) for h in range(2)]

        def cols(b):
            start, size = blocks[b]
            return slice(start, start + size)

        def whole_block(b):
            for half in halves:
                gw_ref[half, cols(b)] = dot(a_t[half], g_at(b)[...]) * scale

        def whole_pair(b):
            start, size = blocks[b]
            for half in halves:
                rhs = jnp.concatenate([g_at(b)[...], g_at(b + 1)[...]], axis=1)
                gw_ref[half, start : start + 2 * size] = dot(a_t[half], rhs) * scale

        def tokens_of(near_side):
            first = (side if near_side else 1 - side) * 2 * chip
            return pl.ds(pl.multiple_of(first, 2 * chip), 2 * chip)

        def rhs_of(b, toks_at):
            if b < full:
                return g_at(b)[toks_at]
            return jnp.concatenate([g_at(b)[toks_at], g_at(b + 1)[toks_at]], axis=1)

        def early_block(b):
            start, toks_at = blocks[b][0], tokens_of(True)
            for half in halves:
                gw_ref[half, start : start + WIDE] = dot(a_t[half, toks_at], rhs_of(b, toks_at))

        def late_block(b):
            start, toks_at = blocks[b][0], tokens_of(False)
            for half in halves:
                term = dot(a_t[half, toks_at], rhs_of(b, toks_at))
                gw_ref[half, start : start + WIDE] = (gw_ref[half, start : start + WIDE] + term) * scale

        def out_at(b):
            return sums_out.at[b - RAW] if b < full else slim_out.at[b - full]

        def in_at(b):
            return sums_in.at[b - RAW] if b < full else slim_in.at[b - full]

        def sum_block(b):
            first = pl.multiple_of((1 - side) * chip, chip)
            for half in halves:
                rhs = g_at(b)[pl.ds(first, (n_line - 1) * chip)]
                out_at(b)[half] = dot(p_t[half], rhs).astype(jnp.bfloat16)
                send(10, out_at(b).at[half], in_at(b).at[half], sum_sem.at[b - RAW], (outward, tp))

        def own_block(b):
            here = pl.ds(pl.multiple_of(z_end * chip, chip), chip)
            for half in halves:
                gw_ref[half, cols(b)] = dot(a_t[half, here], g_at(b)[here])

        def add_block(b):
            landed(in_at(b), sum_sem.at[b - RAW])
            gw_ref[:, cols(b)] = (gw_ref[:, cols(b)] + in_at(b)[...].astype(jnp.float32)) * scale

        if is_mid:
            for c in range(2):
                act_send(2 * z_far_end + c, 2 * z_far_mid + c, ends)
            g_mine(1)
            g_mine(0)
            g_mine(3)
            pass_end(me)
            act_send(2 * z_end + 1 - core, mate, ends)
            spread(ends, me)
            spread(acts, me)
            act_send(mate, mate, acts)
            piece(0)
            piece(1)
            arrive(ends, mate)
            arrive(acts, mate)
            piece(2)
            piece(3)
            piece(4)
            arrive(ends, 2 * z_far_mid + core)
            piece(5)
            piece(6)
            relay(ends, me)
            arrive(ends, 2 * z_far_mid + 1 - core)
            g_take(z_end, FROM_SIDE, 1)
            piece(7)
            relay(acts, me)
            relay(ends, mate)
            arrive(ends, 2 * z_far_end + core)
            relay(acts, mate)
            relay(ends, 2 * z_far_mid + core)
            g_take(z_far_mid, FROM_MID, 1)
            arrive(ends, 2 * z_far_end + 1 - core)
            relay(ends, 2 * z_far_mid + 1 - core)
            relay(ends, 2 * z_far_end + core)
            g_take(z_far_mid, FROM_MID, 0)
            g_take(z_far_mid, FROM_MID, 3)
            turn(ends, z_mid)
            g_take(z_end, FROM_SIDE, 0)
            part_one(0)
            relay(ends, 2 * z_far_end + 1 - core)
            turn(acts, z_mid)
            g_take(z_far_end, FROM_END, 1)
            g_take(z_end, FROM_SIDE, 2)
            g_mine(2)
            g_mates(n_line, 1)
            part_one(1)
            turn(ends, z_far_mid)
            g_take(z_far_end, FROM_END, 0)
            part_two(0)
            turn(ends, z_far_end)
            g_mates(n_line, 0)
            g_take(z_end, FROM_SIDE, 3)
            for c in range(2):
                act_send(2 * z_far_mid + c, 2 * z_far_mid + c, acts)
            sum_block(1)
            g_take(z_far_end, FROM_END, 2)
            part_two(1)
            g_take(z_far_mid, FROM_MID, 2)
            g_take(z_end, FROM_SIDE, 4)
            g_mine(4)
            g_mine(5)
            g_take(z_end, FROM_SIDE, 5)
            g_mine(6)
            part_one(2)
            part_one(3)
            g_mates(n_line, 2)
            sum_block(2)
            g_take(z_far_end, FROM_END, 3)
            part_one(4)
            part_one(5)
            g_mates(n_line, 3)
            sum_block(3)
            arrive(acts, 2 * z_far_mid + core)
            arrive(acts, 2 * z_far_end + core)
            part_two(2)
            part_two(3)
            arrive(acts, 2 * z_far_mid + 1 - core)
            arrive(acts, 2 * z_far_end + 1 - core)
            g_take(z_far_end, FROM_END, 4)
            g_take(z_end, FROM_SIDE, 6)
            g_mine(7)
            g_take(z_end, FROM_SIDE, 7)
            g_mine(8)
            g_take(z_end, FROM_SIDE, 8)
            part_two(4)
            part_one(6)
            part_one(7)
            g_take(z_far_mid, FROM_MID, 4)
            g_mates(n_line, 4)
            sum_block(4)
            g_take(z_far_mid, FROM_MID, 5)
            g_take(z_far_end, FROM_END, 5)
            part_two(5)
            g_mates(n_line, 5)
            sum_block(5)
            relay(acts, 2 * z_far_mid + core)
            g_take(z_far_mid, FROM_MID, 6)
            g_take(z_far_end, FROM_END, 6)
            relay(acts, 2 * z_far_end + core)
            turn_whole(z_end)
            g_mates(n_line, 6)
            sum_block(6)
            relay(acts, 2 * z_far_mid + 1 - core)
            g_take(z_far_mid, FROM_MID, 7)
            g_take(z_far_end, FROM_END, 7)
            relay(acts, 2 * z_far_end + 1 - core)
            early_block(0)
            g_mates(n_line, 7)
            sum_block(7)
            g_take(z_far_mid, FROM_MID, 8)
            g_take(z_far_end, FROM_END, 8)
            early_block(1)
            g_mates(n_line, 8)
            sum_block(8)
            early_block(2)
            early_block(3)
            early_block(5)
            part_two(6)
            turn(acts, z_far_mid)
            turn(acts, z_far_end)
            late_block(0)
            late_block(1)
            part_two(7)
            late_block(2)
            late_block(3)
            late_block(5)
            whole_pair(7)
            part_sum(0)
            part_sum(1)
            part_sum(2)
            part_sum(3)
            part_sum(4)
            part_sum(5)
            part_sum(6)
            part_sum(7)
        else:
            act_send(2 * z_mid + 1 - core, mate, ends)
            spread(ends, me)
            act_send(mate, mate, acts)
            g_mine(1)
            for c in range(2):
                act_send(2 * z_far_end + c, 2 * z_far_mid + c, ends)
            pass_back(me, tp)
            g_mine(0)
            g_mine(2)
            spread(acts, me)
            piece(0)
            piece(1)
            arrive(ends, mate)
            arrive(acts, mate)
            part_one(0)
            piece(2)
            piece(3)
            piece(4)
            piece(5)
            piece(6)
            relay(ends, me)
            g_take(z_mid, FROM_SIDE, 0)
            piece(7)
            part_one(1)
            relay(acts, me)
            part_one(2)
            arrive(acts, 2 * z_mid + core)
            relay(ends, mate)
            arrive(acts, 2 * z_mid + 1 - core)
            part_one(3)
            relay(acts, mate)
            arrive(acts, 2 * z_far_mid + core)
            arrive(acts, 2 * z_far_mid + 1 - core)
            part_one(4)
            part_one(5)
            part_two(0)
            arrive(acts, 2 * z_far_end + core)
            part_one(6)
            gathered(ends, z_end)
            pass_back(me, diag)
            g_mine(7)
            g_mine(3)
            g_mine(5)
            g_mine(8)
            g_mine(4)
            pass_back(me, near)
            for c in range(2):
                act_send(2 * z_far_mid + c, 2 * z_far_mid + c, acts)
            g_mine(6)
            pass_back(mate, near)
            pass_back(me, next_)
            pass_back(mate, diag)
            pass_back(mate, next_)
            pass_back(mate, tp)
            arrive(acts, 2 * z_far_end + 1 - core)
            part_two(1)
            part_one(7)
            turn(acts, z_end)
            g_mates(1, 1)
            own_block(1)
            g_mates(1, 2)
            own_block(2)
            g_mates(1, 3)
            own_block(3)
            g_take(z_far_mid, FROM_MID, 0)
            g_mates(1, 4)
            own_block(4)
            g_mates(1, 5)
            own_block(5)
            relay(acts, 2 * z_mid + core)
            g_mates(1, 6)
            own_block(6)
            g_mates(1, 7)
            own_block(7)
            g_mates(1, 8)
            own_block(8)
            part_two(2)
            relay(acts, 2 * z_mid + 1 - core)
            part_sum(0)
            part_two(3)
            relay(acts, 2 * z_far_mid + core)
            g_take(z_far_end, FROM_END, 0)
            relay(acts, 2 * z_far_mid + 1 - core)
            part_sum(1)
            g_mates(n_line, 0)
            part_sum(2)
            part_two(4)
            turn(acts, z_mid)
            add_block(1)
            part_sum(3)
            part_two(5)
            relay(acts, 2 * z_far_end + core)
            turn(acts, z_far_mid)
            part_sum(4)
            part_two(6)
            add_block(2)
            relay(acts, 2 * z_far_end + 1 - core)
            part_sum(5)
            add_block(3)
            part_two(7)
            part_sum(6)
            turn(acts, z_far_end)
            whole_block(0)
            add_block(4)
            part_sum(7)
            add_block(5)
            add_block(6)
            add_block(7)
            add_block(8)
        all_sent()

    is_mid = z == z_mid

    @pl.when(is_mid)
    def _():
        program(True)

    @pl.when(jnp.logical_not(is_mid))
    def _():
        program(False)


def square_body(act_codes, scale_exps, weight, grad_out):
    n_ctx, n_tp = lax.axis_size("ctx"), lax.axis_size("tp")
    rows, width = act_codes.shape
    toks, cols = grad_out.shape
    feats = width // n_ctx
    d_tile = width // 8
    n_d = width // d_tile
    all_toks = toks * n_ctx
    n_b = len(blocks_of(cols))
    full = wide_blocks(cols)
    dma = pltpu.SemaphoreType.DMA
    vmem = pl.BlockSpec(memory_space=pltpu.VMEM)
    hbm = pl.BlockSpec(memory_space=pltpu.HBM)
    bf16 = jnp.bfloat16
    outs = rows * width * 2 + feats * cols * 4
    gin, gw = pl.pallas_call(
        functools.partial(square_kernel, n_ctx, n_tp, all_toks),
        out_shape=(
            pltpu.VMEM((rows, width), bf16),
            pltpu.VMEM((feats, cols), jnp.float32),
        ),
        in_specs=[hbm, hbm, hbm, hbm],
        out_specs=(vmem, vmem),
        scratch_shapes=[
            pltpu.VMEM((rows, width), bf16),
            pltpu.VMEM(scale_exps.shape[::-1], scale_exps.dtype),
            pltpu.VMEM((n_d, d_tile, cols), bf16),
            pltpu.VMEM((toks, cols), bf16),
            pltpu.VMEM((full, all_toks, WIDE), bf16),
            pltpu.VMEM((n_b - full, all_toks, WIDE // 2), bf16),
            pltpu.VMEM((n_ctx, rows, feats), bf16),
            pltpu.VMEM((n_ctx, n_tp, rows, feats), bf16),
            pltpu.VMEM((n_ctx, n_tp, rows, feats), bf16),
            pltpu.VMEM((feats, all_toks), bf16),
            pltpu.VMEM((feats, all_toks - 2 * toks), bf16),
            pltpu.VMEM((n_d, n_tp, rows, d_tile), bf16),
            pltpu.VMEM((n_d, 2, rows, d_tile), bf16),
            pltpu.VMEM((n_d, rows, d_tile), bf16),
            pltpu.VMEM((n_d, rows, d_tile), bf16),
            pltpu.VMEM((max(full - RAW, 1), feats, WIDE), bf16),
            pltpu.VMEM((max(full - RAW, 1), feats, WIDE), bf16),
            pltpu.VMEM((n_b - full, feats, WIDE // 2), bf16),
            pltpu.VMEM((n_b - full, feats, WIDE // 2), bf16),
            dma((4,)),
            dma((2,)),
            dma((11,)),
            dma((2, n_ctx)),
            dma((2, n_ctx)),
            dma((2, n_ctx // 2)),
            dma((3, n_b)),
            dma((n_b,)),
            dma((n_d,)),
            dma((n_d,)),
            dma((n_b - RAW,)),
        ],
        compiler_params=pltpu.CompilerParams(
            collective_id=0, has_side_effects=True, vmem_limit_bytes=67_043_328 - outs - 8192
        ),
    )(act_codes, scale_exps.T, weight, grad_out)
    return pl.pallas_call(
        store_kernel,
        out_shape=(
            jax.ShapeDtypeStruct(gin.shape, gin.dtype), jax.ShapeDtypeStruct(gw.shape, gw.dtype)
        ),
        in_specs=[vmem, vmem],
        out_specs=(hbm, hbm),
        scratch_shapes=[dma((2,))],
        compiler_params=pltpu.CompilerParams(vmem_limit_bytes=1 << 20),
    )(gin, gw)


def store_kernel(gin_ref, gw_ref, gin_out, gw_out, sem):
    copies = [
        pltpu.make_async_copy(gw_ref, gw_out, sem.at[0]),
        pltpu.make_async_copy(gin_ref, gin_out, sem.at[1]),
    ]
    for copy in copies:
        copy.start()
    for copy in copies:
        copy.wait()


def body(act_codes, scale_exps, weight, grad_out):
    line, square = lax.axis_size("ctx") // 2, lax.axis_size("tp")
    if line == 4 and square == 4 and grad_out.shape[1] % WIDE == 0:
        return square_body(act_codes, scale_exps, weight, grad_out)
    return line_body(act_codes, scale_exps, weight, grad_out)


def solution(mesh):
    placed = (P(("ctx", "tp"), None), P(("ctx", "tp"), None), P(None, "tp"), P("ctx", "tp"))
    return jax.shard_map(
        body,
        mesh=mesh,
        in_specs=placed,
        out_specs=(P(("ctx", "tp"), None), P("ctx", "tp")),
        check_vma=False,
    )
```
